128 devices in a mesh: data: 1, expert: 128 (over z, y, x, core).
Axes of the slice: x: 4, y: 4, z: 4, core: 2. Of those that a mesh axis runs over, the one named last changes fastest.
Arguments:
- token_rows: bfloat16 [65536, 1024], P(('data', 'expert'))
- expert_ids: int32 [65536, 2], P(('data', 'expert'))
- gate_weights: float32 [65536, 2], P(('data', 'expert'))
- w_in: bfloat16 [128, 1024, 1024], P('expert')
- w_out: bfloat16 [128, 1024, 1024], P('expert')
Outputs:
- output: bfloat16 [65536, 1024], P(('data', 'expert'))
All inputs are finite; a program needn't handle non-finite values.
Results may differ from the reference program's by a relative error of at most 0.001.
Values are sent between devices in bfloat16 or wider.
A program may use at most 1 GiB of HBM per device.

```python
import math
import jax
import jax.numpy as jnp
from jax import lax

TOKENS_DEV = 512
GROUP_DEVS = 128
MODEL_DIM = 1024
HIDDEN_DIM = 1024
EXPERTS = 128
TOP_K = 2

TOKENS = TOKENS_DEV * GROUP_DEVS
MEAN_LOAD = TOKENS_DEV * TOP_K // EXPERTS
CAPACITY = TOKENS * TOP_K // EXPERTS
POP_SPREAD = MEAN_LOAD // 2
DEV_SPREAD = MEAN_LOAD // 4


def draw_routing(key):
    key_order, key_pop, key_dev, key_tok, key_col = jax.random.split(key, 5)
    expert_order = jax.random.permutation(key_order, EXPERTS)
    pop_bias = jax.random.randint(key_pop, (EXPERTS,), 0, POP_SPREAD + 1)
    pop_bias = pop_bias.at[0].set(POP_SPREAD).at[1].set(0)
    dev_bias = jax.random.randint(key_dev, (GROUP_DEVS, EXPERTS), 0, DEV_SPREAD + 1)
    dev_bias = dev_bias.at[:, 0].set(DEV_SPREAD).at[:, 1].set(0)
    pair_load = MEAN_LOAD + (pop_bias - jnp.roll(pop_bias, -1))[None, :] + dev_bias - jnp.roll(dev_bias, -1, axis=1)
    run_ends = jnp.cumsum(pair_load, axis=1)
    positions = jnp.arange(TOKENS_DEV * TOP_K, dtype=jnp.int32)

    def find_run(row_ends):
        return jnp.searchsorted(row_ends, positions, side="right")

    run_index = jax.vmap(find_run)(run_ends)
    labels = expert_order[run_index].reshape(GROUP_DEVS, TOP_K, TOKENS_DEV)
    choices = jnp.swapaxes(labels, 1, 2)

    def token_order(sub_key):
        return jax.random.permutation(sub_key, TOKENS_DEV)

    tok_perm = jax.vmap(token_order)(jax.random.split(key_tok, GROUP_DEVS))
    choices = jnp.take_along_axis(choices, tok_perm[:, :, None], axis=1)
    choices = jax.random.permutation(key_col, choices, axis=2, independent=True)
    return choices.reshape(TOKENS, TOP_K).astype(jnp.int32)


def draw_matrices(key, fan_in, fan_out):
    def one_matrix(sub_key):
        return (jax.random.normal(sub_key, (fan_in, fan_out), jnp.float32) / math.sqrt(fan_in)).astype(jnp.bfloat16)
    return lax.map(one_matrix, jax.random.split(key, EXPERTS))


def setup_inputs(seed: int = 0, part: int = 0) -> dict:
    root = jax.random.key(seed)
    part_key = jax.random.fold_in(root, part)
    key_route, key_rows, key_gate = jax.random.split(part_key, 3)
    key_up, key_down = jax.random.split(jax.random.fold_in(root, 1000003), 2)
    token_rows = jax.random.normal(key_rows, (TOKENS, MODEL_DIM), jnp.float32).astype(jnp.bfloat16)
    gate_weights = jax.random.uniform(key_gate, (TOKENS, TOP_K), jnp.float32, 0.5, 1.5) / math.sqrt(TOP_K)
    return {"token_rows": token_rows, "expert_ids": draw_routing(key_route), "gate_weights": gate_weights, "w_in": draw_matrices(key_up, MODEL_DIM, HIDDEN_DIM), "w_out": draw_matrices(key_down, HIDDEN_DIM, MODEL_DIM)}


def expert_ffn(operands):
    rows, up_weight, down_weight = operands
    hidden = jax.nn.gelu(jnp.dot(rows, up_weight, preferred_element_type=jnp.float32)).astype(jnp.bfloat16)
    return jnp.dot(hidden, down_weight, preferred_element_type=jnp.float32).astype(jnp.bfloat16)


def reference(token_rows, expert_ids, gate_weights, w_in, w_out):
    pairs = TOP_K * TOKENS
    flat_ids = expert_ids.T.reshape(pairs)
    sort_order = jnp.argsort(flat_ids, stable=True)
    position = jnp.zeros((pairs,), jnp.int32).at[sort_order].set(jnp.arange(pairs, dtype=jnp.int32))
    counts = jnp.bincount(flat_ids, length=EXPERTS)
    seg_start = jnp.cumsum(counts) - counts
    slot = position - seg_start[flat_ids]
    keep = slot < CAPACITY
    slot_safe = jnp.where(keep, slot, CAPACITY)
    buffer = jnp.zeros((EXPERTS, CAPACITY, MODEL_DIM), token_rows.dtype).at[flat_ids, slot_safe].set(jnp.tile(token_rows, (TOP_K, 1)), mode="drop")
    outputs = lax.map(expert_ffn, (buffer, w_in, w_out))
    weight = jnp.where(keep, gate_weights.T.reshape(pairs), 0.0).reshape(TOP_K, TOKENS)
    slot_read = jnp.minimum(slot, CAPACITY - 1).reshape(TOP_K, TOKENS)

    def add_choice(total, pieces):
        choice_weight, choice_ids, choice_slot = pieces
        return total + choice_weight[:, None] * outputs[choice_ids, choice_slot].astype(jnp.float32), None

    mixed, _ = lax.scan(add_choice, token_rows.astype(jnp.float32), (weight, flat_ids.reshape(TOP_K, TOKENS), slot_read))
    return mixed.astype(jnp.bfloat16)
```

```python
import functools

import jax
import jax.numpy as jnp
from jax import lax
from jax.experimental import pallas as pl
from jax.experimental.pallas import tpu as pltpu
from jax.sharding import PartitionSpec as P

SLOTS = 14
WIRE_ROWS = 16
BF16 = jnp.bfloat16
F32 = jnp.float32
I32 = jnp.int32


def moe_kernel(dims, capacity, ids_row, ids_col, gates, x, win_hbm, wout_hbm, out,
               outbuf, inbuf, obuf, retbuf, cbuf, win, wout, st, xs, hs, acc0, acc1, tmat, tinv, rrow, rcol, wcol,
               w_sem, c_send, c_recv, d_send, d_recv, r_send, r_recv):
    nz, ny, nx, nk = dims
    n = nz * ny * nx * nk
    nc, ng = nz * ny, nx * nk
    tokens, model = x.shape
    hidden = win.shape[1]
    dense = SLOTS * nc
    wire = WIRE_ROWS * nc
    half, quarter, eighth = model // 2, model // 4, model // 8
    width = SLOTS * model // WIRE_ROWS
    me = lax.axis_index("expert")
    mk = me % nk
    mx = (me // nk) % nx
    my = (me // (nk * nx)) % ny
    mz = me // (nk * nx * ny)

    def peer(g, c, sign):
        dx, dk, dz, dy = g // nk, g % nk, c // ny, c % ny
        z = (mz + nz + sign * dz) % nz
        y = (my + ny + sign * dy) % ny
        xx = (mx + nx + sign * dx) % nx
        k = (mk + nk + sign * dk) % nk
        return ((z * ny + y) * nx + xx) * nk + k

    def chunk_copy(src, dst, ssem, rsem, g, c, sign):
        rows = pl.ds(pl.multiple_of(g * wire + c * WIRE_ROWS, WIRE_ROWS), WIRE_ROWS)
        return pltpu.make_async_remote_copy(src_ref=src.at[rows], dst_ref=dst.at[rows], send_sem=ssem.at[g], recv_sem=rsem.at[g],
                                            device_id={"expert": peer(g, c, sign)}, device_id_type=pl.DeviceIdType.MESH)

    def start_group(src, dst, ssem, rsem, g, sign):
        def one(c, carry):
            @pl.when(g + c > 0)
            def _():
                chunk_copy(src, dst, ssem, rsem, g, c, sign).start()
            return carry
        lax.fori_loop(0, nc, one, 0)

    def wait_group(src, dst, ssem, rsem, g, recv):
        def wait(first, count):
            rows = pl.ds(pl.multiple_of(first, WIRE_ROWS), count)
            copy = pltpu.make_async_remote_copy(src_ref=src.at[rows], dst_ref=dst.at[rows], send_sem=ssem.at[g], recv_sem=rsem.at[g],
                                                device_id={"expert": me}, device_id_type=pl.DeviceIdType.MESH)
            copy.wait_recv() if recv else copy.wait_send()

        @pl.when(g == 0)
        def _():
            wait(WIRE_ROWS, wire - WIRE_ROWS)

        @pl.when(g > 0)
        def _():
            wait(g * wire, wire)

    def row_of(ids, slot):
        dz = (ids // (nk * nx * ny) + nz - mz) % nz
        dy = ((ids // (nk * nx)) % ny + ny - my) % ny
        dx = ((ids // nk) % nx + nx - mx) % nx
        dk = (ids % nk + nk - mk) % nk
        return (dx * nk + dk) * dense + slot * nc + dz * ny + dy

    def iota(shape, dim):
        return lax.broadcasted_iota(I32, shape, dim)

    def ones(mask):
        return jnp.where(mask, jnp.float32(1.0), jnp.float32(0.0)).astype(BF16)

    weights_in = pltpu.make_async_copy(win_hbm.at[0], win, w_sem.at[0])
    weights_out = pltpu.make_async_copy(wout_hbm.at[0], wout, w_sem.at[1])
    weights_in.start()
    weights_out.start()

    lanes = iota((tokens, n), 1)
    count = [jnp.sum(jnp.where(ids_col[:, j:j + 1] == lanes, 1, 0).astype(I32), axis=0, keepdims=True) for j in range(2)]
    cbuf[0] = count[0] + count[1] * 65536

    def count_copy(g, c):
        slot = g * nc + c
        return pltpu.make_async_remote_copy(src_ref=cbuf.at[0], dst_ref=cbuf.at[slot], send_sem=c_send.at[0], recv_sem=c_recv.at[0],
                                            device_id={"expert": peer(g, c, 1)}, device_id_type=pl.DeviceIdType.MESH)

    def send_counts(i, carry):
        count_copy(i // nc, i % nc).start()
        return carry
    lax.fori_loop(1, n, send_counts, 0)

    earlier = iota((tokens, tokens), 0) < iota((tokens, tokens), 1)
    row_ids = [ids_row[j:j + 1, :] for j in range(2)]

    def lane_rank(j, other, mask):
        same = ids_col[:, j:j + 1] == row_ids[other]
        if mask:
            same = same & earlier
        return jnp.sum(jnp.where(same, 1, 0).astype(I32), axis=0, keepdims=True)
    rrow[0:1, :] = row_of(row_ids[0], lane_rank(0, 0, True))
    rrow[1:2, :] = row_of(row_ids[1], lane_rank(1, 1, True) + lane_rank(0, 1, False))

    swap = (iota((wire, wire), 0) % WIRE_ROWS) * nc + iota((wire, wire), 0) // WIRE_ROWS
    tmat[...] = ones(swap == iota((wire, wire), 1))
    swap = (iota((wire, wire), 1) % WIRE_ROWS) * nc + iota((wire, wire), 1) // WIRE_ROWS
    tinv[...] = ones(swap == iota((wire, wire), 0))

    step = quarter

    def stack(b, block):
        h, r = (b * quarter) // half, (b * quarter) % half
        st[h * 8 * nc:(h + 1) * 8 * nc, r:r + quarter] = block[:8 * nc]
        st[b * 4 * nc:(b + 1) * 4 * nc, half:half + quarter] = block[8 * nc:12 * nc]
        for o in range(2):
            st[(2 * b + o) * 2 * nc:(2 * b + o + 1) * 2 * nc, half + quarter:width] = block[12 * nc:, o * eighth:(o + 1) * eighth]

    def to_wire(buf, g):
        rows = pl.ds(pl.multiple_of(g * wire, WIRE_ROWS), wire)
        for lo, hi in ((0, quarter), (quarter, half), (half, half + quarter), (half + quarter, width)):
            buf[rows, lo:hi] = jnp.dot(tmat[...], st[:, lo:hi], preferred_element_type=F32).astype(BF16)

    def from_wire(buf, g, dst):
        rows = pl.ds(pl.multiple_of(g * wire, WIRE_ROWS), wire)
        for r in (0, quarter):
            part = jnp.dot(tinv[...], buf[rows, r:r + quarter], preferred_element_type=F32).astype(BF16)
            dst[0:8 * nc, r:r + quarter] = part[:8 * nc]
            dst[0:8 * nc, half + r:half + r + quarter] = part[8 * nc:]
        part = jnp.dot(tinv[...], buf[rows, half:half + quarter], preferred_element_type=F32).astype(BF16)
        for q in range(4):
            dst[8 * nc:12 * nc, q * quarter:(q + 1) * quarter] = part[q * 4 * nc:(q + 1) * 4 * nc]
        part = jnp.dot(tinv[...], buf[rows, half + quarter:width], preferred_element_type=F32).astype(BF16)
        for o in range(8):
            dst[12 * nc:dense, o * eighth:(o + 1) * eighth] = part[o * 2 * nc:(o + 1) * 2 * nc]

    def dispatch(g, carry):
        rows = iota((dense, tokens), 0) + g * dense
        pick = ones((rows == rrow[0:1, :]) | (rows == rrow[1:2, :]))
        for b in range(4):
            block = jnp.dot(pick, x[:, b * step:(b + 1) * step], preferred_element_type=F32).astype(BF16)
            stack(b, block)
        to_wire(outbuf, g)
        start_group(outbuf, inbuf, d_send, d_recv, g, 1)
        return carry
    lax.fori_loop(0, ng, dispatch, 0)
    inbuf[0:WIRE_ROWS, :] = outbuf[0:WIRE_ROWS, :]

    later = iota((tokens, tokens), 1) < iota((tokens, tokens), 0)

    def sub_rank(j, other, mask):
        same = ids_col[:, other:other + 1] == row_ids[j]
        if mask:
            same = same & later
        return jnp.sum(jnp.where(same, 1, 0).astype(I32), axis=1, keepdims=True)
    rank0 = sub_rank(0, 0, True)
    rank1 = sub_rank(1, 1, True)
    rcol[:, 0:1] = row_of(ids_col[:, 0:1], rank0)
    rcol[:, 1:2] = row_of(ids_col[:, 1:2], rank1 + sub_rank(0, 1, False))
    rcol[:, 2:3] = rank0
    rcol[:, 3:4] = rank1

    weights_in.wait()
    weights_out.wait()

    def expert(g, carry):
        wait_group(outbuf, inbuf, d_send, d_recv, g, True)
        from_wire(inbuf, g, xs)
        for b in range(4):
            cols = slice(b * hidden // 4, (b + 1) * hidden // 4)
            pre = jnp.dot(xs[0:dense, :], win[:, cols], preferred_element_type=F32)
            hs[:, cols] = jax.nn.gelu(pre).astype(BF16)
        for b in range(4):
            block = jnp.dot(hs[...], wout[:, b * step:(b + 1) * step], preferred_element_type=F32).astype(BF16)
            stack(b, block)
        to_wire(obuf, g)
        start_group(obuf, retbuf, r_send, r_recv, g, -1)
        return carry
    lax.fori_loop(0, ng, expert, 0)
    retbuf[0:WIRE_ROWS, :] = obuf[0:WIRE_ROWS, :]

    pltpu.make_async_remote_copy(src_ref=cbuf.at[pl.ds(1, n - 1)], dst_ref=cbuf.at[pl.ds(1, n - 1)], send_sem=c_send.at[0], recv_sem=c_recv.at[0],
                                 device_id={"expert": me}, device_id_type=pl.DeviceIdType.MESH).wait()

    def add_counts(i, carry):
        before0, before1, total0 = carry
        packed = cbuf[i]
        second = packed // 65536
        first = packed - second * 65536
        use = jnp.where(peer(i // nc, i % nc, -1) < me, 1, 0).astype(I32)
        return before0 + first * use, before1 + second * use, total0 + first
    zero = jnp.zeros((1, n), I32)
    before0, before1, total0 = lax.fori_loop(0, n, add_counts, (zero, zero, zero))
    for j, offset in enumerate((before0, total0 + before1)):
        mine = jnp.sum(jnp.where(ids_col[:, j:j + 1] == lanes, offset, 0), axis=1, keepdims=True)
        wcol[:, j:j + 1] = jnp.where(mine + rcol[:, 2 + j:3 + j] < capacity, gates[:, j:j + 1], 0.0)

    acc0[...] = jnp.zeros_like(acc0)
    acc1[...] = jnp.zeros_like(acc1)
    xs[dense:wire, :] = jnp.zeros((wire - dense, model), BF16)

    def combine(g, carry):
        wait_group(obuf, retbuf, r_send, r_recv, g, True)
        from_wire(retbuf, g, xs)
        cols = iota((tokens, wire), 1)
        for j, acc in enumerate((acc0, acc1)):
            want = rcol[:, j:j + 1] - g * dense
            pick = ones((want == cols) & (cols < dense))
            for b in range(4):
                part = slice(b * step, (b + 1) * step)
                acc[:, part] += jnp.dot(pick, xs[:, part], preferred_element_type=F32)
        return carry
    lax.fori_loop(0, ng, combine, 0)
    out[...] = (x[...].astype(F32) + wcol[:, 0:1] * acc0[...] + wcol[:, 1:2] * acc1[...]).astype(BF16)

    def drain(g, carry):
        wait_group(outbuf, inbuf, d_send, d_recv, g, False)
        wait_group(obuf, retbuf, r_send, r_recv, g, False)
        return carry
    lax.fori_loop(0, ng, drain, 0)


def torus(n):
    return (4, 4, 4, 2) if n == 128 else (2, n // 4, 1, 2)


def solution(mesh):
    n = mesh.shape["expert"]
    row_spec = P(("data", "expert"), None)
    weight_spec = P("expert", None, None)
    dims = torus(n)

    def device_step(token_rows, expert_ids, gate_weights, w_in, w_out):
        tokens, model = token_rows.shape
        hidden = w_in.shape[2]
        nc, ng = dims[0] * dims[1], dims[2] * dims[3]
        wire, dense = nc * WIRE_ROWS, nc * SLOTS
        width = SLOTS * model // WIRE_ROWS
        capacity = n * (tokens * 2 // n)
        vmem = pl.BlockSpec(memory_space=pltpu.VMEM)
        hbm = pl.BlockSpec(memory_space=pl.ANY)
        dma = pltpu.SemaphoreType.DMA
        return pl.pallas_call(
            functools.partial(moe_kernel, dims, capacity),
            out_shape=jax.ShapeDtypeStruct((tokens, model), BF16),
            in_specs=[vmem, vmem, vmem, vmem, hbm, hbm],
            out_specs=vmem,
            scratch_shapes=[
                pltpu.VMEM((ng * wire, width), BF16),
                pltpu.VMEM((ng * wire, width), BF16),
                pltpu.VMEM((ng * wire, width), BF16),
                pltpu.VMEM((ng * wire, width), BF16),
                pltpu.VMEM((n, 1, n), I32),
                pltpu.VMEM((model, hidden), BF16),
                pltpu.VMEM((hidden, model), BF16),
                pltpu.VMEM((wire, width), BF16),
                pltpu.VMEM((wire, model), BF16),
                pltpu.VMEM((dense, hidden), BF16),
                pltpu.VMEM((tokens, model), F32),
                pltpu.VMEM((tokens, model), F32),
                pltpu.VMEM((wire, wire), BF16),
                pltpu.VMEM((wire, wire), BF16),
                pltpu.VMEM((2, tokens), I32),
                pltpu.VMEM((tokens, 4), I32),
                pltpu.VMEM((tokens, 2), F32),
                dma((2,)), dma((1,)), dma((1,)), dma((ng,)), dma((ng,)), dma((ng,)), dma((ng,)),
            ],
            compiler_params=pltpu.CompilerParams(has_side_effects=True, vmem_limit_bytes=60 * 1024 * 1024),
        )(expert_ids.T, expert_ids, gate_weights, token_rows, w_in, w_out)

    return jax.shard_map(device_step, mesh=mesh, in_specs=(row_spec, row_spec, row_spec, weight_spec, weight_spec), out_specs=row_spec, check_vma=False)
```

```python
import functools

import jax
import jax.numpy as jnp
from jax import lax
from jax.experimental import pallas as pl
from jax.experimental.pallas import tpu as pltpu
from jax.sharding import PartitionSpec as P

SLOTS = 14
WIRE_ROWS = 16
BF16 = jnp.bfloat16
F32 = jnp.float32
I32 = jnp.int32


def moe_kernel(dims, capacity, ids_row, gates_row, x, win_hbm, wout_hbm, out,
               outbuf, inbuf, obuf, retbuf, cbuf, win, wout, st, xs, hs, acc0, acc1, tmat, tinv, rrow, rcol, wcol, flat, turned,
               w_sem, c_send, c_recv, d_send, d_recv, r_send, r_recv):
    nz, ny, nx, nk = dims
    n = nz * ny * nx * nk
    nc, ng = nz * ny, nx * nk
    tokens, model = x.shape
    hidden = win.shape[1]
    dense = SLOTS * nc
    wire = WIRE_ROWS * nc
    half, quarter, eighth = model // 2, model // 4, model // 8
    width = SLOTS * model // WIRE_ROWS
    me = lax.axis_index("expert")
    mk = lax.rem(me, nk)
    mx = lax.rem(lax.div(me, nk), nx)
    my = lax.rem(lax.div(me, nk * nx), ny)
    mz = lax.div(me, nk * nx * ny)

    def digits(sign):
        zs = [lax.rem(mz + nz + sign * d, nz) * (ny * nx * nk) for d in range(nz)]
        ys = [lax.rem(my + ny + sign * d, ny) * (nx * nk) for d in range(ny)]
        return [zs[c // ny] + ys[c % ny] for c in range(nc)]
    ahead, behind = digits(1), digits(-1)

    def base_of(g, sign):
        dx, dk = lax.div(g, nk), lax.rem(g, nk)
        return lax.rem(mx + nx + sign * dx, nx) * nk + lax.rem(mk + nk + sign * dk, nk)

    def each_peer(g, sign, act):
        base = base_of(g, sign)
        for c in range(nc):
            device = (ahead if sign > 0 else behind)[c] + base
            if c > 0:
                act(c, device)
            else:
                @pl.when(g > 0)
                def _():
                    act(c, device)

    def start_group(src, dst, ssem, rsem, g, sign):
        def act(c, device):
            rows = pl.ds(pl.multiple_of(g * wire + c * WIRE_ROWS, WIRE_ROWS), WIRE_ROWS)
            pltpu.make_async_remote_copy(src_ref=src.at[rows], dst_ref=dst.at[rows], send_sem=ssem.at[g], recv_sem=rsem.at[g],
                                         device_id={"expert": device}, device_id_type=pl.DeviceIdType.MESH).start()
        each_peer(g, sign, act)

    def wait_group(src, dst, ssem, rsem, g, recv):
        def wait(first, count):
            rows = pl.ds(pl.multiple_of(first, WIRE_ROWS), count)
            copy = pltpu.make_async_remote_copy(src_ref=src.at[rows], dst_ref=dst.at[rows], send_sem=ssem.at[g], recv_sem=rsem.at[g],
                                                device_id={"expert": me}, device_id_type=pl.DeviceIdType.MESH)
            copy.wait_recv() if recv else copy.wait_send()

        @pl.when(g == 0)
        def _():
            wait(WIRE_ROWS, wire - WIRE_ROWS)

        @pl.when(g > 0)
        def _():
            wait(g * wire, wire)

    def row_of(ids, slot):
        dz = (ids // (nk * nx * ny) + nz - mz) % nz
        dy = ((ids // (nk * nx)) % ny + ny - my) % ny
        dx = ((ids // nk) % nx + nx - mx) % nx
        dk = (ids % nk + nk - mk) % nk
        return (dx * nk + dk) * dense + slot * nc + dz * ny + dy

    def iota(shape, dim):
        return lax.broadcasted_iota(I32, shape, dim)

    def ones(mask):
        return jnp.where(mask, jnp.float32(1.0), jnp.float32(0.0)).astype(BF16)

    barrier = pltpu.get_barrier_semaphore()

    def hello(g, carry):
        def act(c, device):
            pl.semaphore_signal(barrier, inc=1, device_id={"expert": device}, device_id_type=pl.DeviceIdType.MESH)
        each_peer(g, 1, act)
        return carry
    lax.fori_loop(0, ng, hello, 0)

    weights_in = pltpu.make_async_copy(win_hbm.at[0], win, w_sem.at[0])
    weights_out = pltpu.make_async_copy(wout_hbm.at[0], wout, w_sem.at[1])
    weights_in.start()
    weights_out.start()

    flat[0:2, :] = ids_row[...].astype(F32)
    flat[2:4, :] = gates_row[...]
    flat[4:8, :] = jnp.zeros((4, tokens), F32)
    turned[...] = flat[...].T
    ids_col = turned[:, 0:2].astype(I32)

    earlier = iota((tokens, tokens), 0) < iota((tokens, tokens), 1)
    row_ids = [ids_row[j:j + 1, :] for j in range(2)]

    def lane_rank(j, other, mask):
        same = ids_col[:, j:j + 1] == row_ids[other]
        if mask:
            same = same & earlier
        return jnp.sum(jnp.where(same, 1, 0).astype(I32), axis=0, keepdims=True)
    rrow[0:1, :] = row_of(row_ids[0], lane_rank(0, 0, True))
    rrow[1:2, :] = row_of(row_ids[1], lane_rank(1, 1, True) + lane_rank(0, 1, False))

    swap = (iota((wire, wire), 0) % WIRE_ROWS) * nc + iota((wire, wire), 0) // WIRE_ROWS
    tmat[...] = ones(swap == iota((wire, wire), 1))
    swap = (iota((wire, wire), 1) % WIRE_ROWS) * nc + iota((wire, wire), 1) // WIRE_ROWS
    tinv[...] = ones(swap == iota((wire, wire), 0))

    step = quarter

    def stack(b, block):
        h, r = (b * quarter) // half, (b * quarter) % half
        st[h * 8 * nc:(h + 1) * 8 * nc, r:r + quarter] = block[:8 * nc]
        st[b * 4 * nc:(b + 1) * 4 * nc, half:half + quarter] = block[8 * nc:12 * nc]
        for o in range(2):
            st[(2 * b + o) * 2 * nc:(2 * b + o + 1) * 2 * nc, half + quarter:width] = block[12 * nc:, o * eighth:(o + 1) * eighth]

    def to_wire(buf, g):
        rows = pl.ds(pl.multiple_of(g * wire, WIRE_ROWS), wire)
        for lo, hi in ((0, quarter), (quarter, half), (half, half + quarter), (half + quarter, width)):
            buf[rows, lo:hi] = jnp.dot(tmat[...], st[:, lo:hi], preferred_element_type=F32).astype(BF16)

    def from_wire(buf, g, dst):
        rows = pl.ds(pl.multiple_of(g * wire, WIRE_ROWS), wire)
        for r in (0, quarter):
            part = jnp.dot(tinv[...], buf[rows, r:r + quarter], preferred_element_type=F32).astype(BF16)
            dst[0:8 * nc, r:r + quarter] = part[:8 * nc]
            dst[0:8 * nc, half + r:half + r + quarter] = part[8 * nc:]
        part = jnp.dot(tinv[...], buf[rows, half:half + quarter], preferred_element_type=F32).astype(BF16)
        for q in range(4):
            dst[8 * nc:12 * nc, q * quarter:(q + 1) * quarter] = part[q * 4 * nc:(q + 1) * 4 * nc]
        part = jnp.dot(tinv[...], buf[rows, half + quarter:width], preferred_element_type=F32).astype(BF16)
        for o in range(8):
            dst[12 * nc:dense, o * eighth:(o + 1) * eighth] = part[o * 2 * nc:(o + 1) * 2 * nc]

    def build(g, carry):
        rows = iota((dense, tokens), 0) + g * dense
        pick = ones((rows == rrow[0:1, :]) | (rows == rrow[1:2, :]))
        for b in range(4):
            block = jnp.dot(pick, x[:, b * step:(b + 1) * step], preferred_element_type=F32).astype(BF16)
            stack(b, block)
        to_wire(outbuf, g)
        return carry
    lax.fori_loop(0, ng, build, 0)

    lanes = iota((tokens, n), 1)
    count = [jnp.sum(jnp.where(ids_col[:, j:j + 1] == lanes, 1, 0).astype(I32), axis=0, keepdims=True) for j in range(2)]
    cbuf[0] = count[0] + count[1] * 65536

    pl.semaphore_wait(barrier, n - 1)

    def dispatch(g, carry):
        start_group(outbuf, inbuf, d_send, d_recv, g, 1)
        return carry
    lax.fori_loop(0, ng, dispatch, 0)

    def send_counts(g, carry):
        def act(c, device):
            pltpu.make_async_remote_copy(src_ref=cbuf.at[0], dst_ref=cbuf.at[g * nc + c], send_sem=c_send.at[0], recv_sem=c_recv.at[0],
                                         device_id={"expert": device}, device_id_type=pl.DeviceIdType.MESH).start()
        each_peer(g, 1, act)
        return carry
    lax.fori_loop(0, ng, send_counts, 0)
    inbuf[0:WIRE_ROWS, :] = outbuf[0:WIRE_ROWS, :]

    later = iota((tokens, tokens), 1) < iota((tokens, tokens), 0)

    def sub_rank(j, other, mask):
        same = ids_col[:, other:other + 1] == row_ids[j]
        if mask:
            same = same & later
        return jnp.sum(jnp.where(same, 1, 0).astype(I32), axis=1, keepdims=True)
    rank0 = sub_rank(0, 0, True)
    rank1 = sub_rank(1, 1, True)
    rcol[:, 0:1] = row_of(ids_col[:, 0:1], rank0)
    rcol[:, 1:2] = row_of(ids_col[:, 1:2], rank1 + sub_rank(0, 1, False))
    rcol[:, 2:3] = rank0
    rcol[:, 3:4] = rank1

    weights_in.wait()
    weights_out.wait()

    def expert(g, carry):
        wait_group(outbuf, inbuf, d_send, d_recv, g, True)
        from_wire(inbuf, g, xs)
        for b in range(4):
            cols = slice(b * hidden // 4, (b + 1) * hidden // 4)
            pre = jnp.dot(xs[0:dense, :], win[:, cols], preferred_element_type=F32)
            hs[:, cols] = jax.nn.gelu(pre).astype(BF16)
        for b in range(4):
            block = jnp.dot(hs[...], wout[:, b * step:(b + 1) * step], preferred_element_type=F32).astype(BF16)
            stack(b, block)
        to_wire(obuf, g)
        start_group(obuf, retbuf, r_send, r_recv, g, -1)
        return carry
    lax.fori_loop(0, ng, expert, 0)
    retbuf[0:WIRE_ROWS, :] = obuf[0:WIRE_ROWS, :]

    pltpu.make_async_remote_copy(src_ref=cbuf.at[pl.ds(1, n - 1)], dst_ref=cbuf.at[pl.ds(1, n - 1)], send_sem=c_send.at[0], recv_sem=c_recv.at[0],
                                 device_id={"expert": me}, device_id_type=pl.DeviceIdType.MESH).wait()

    packed = cbuf[...].reshape(n, n)
    second = packed // 65536
    first = packed - second * 65536
    slot = iota((n, n), 0)
    dx, dk, dz, dy = (slot // nc) // nk, (slot // nc) % nk, (slot % nc) // ny, (slot % nc) % ny
    source = (((mz + nz - dz) % nz * ny + (my + ny - dy) % ny) * nx + (mx + nx - dx) % nx) * nk + (mk + nk - dk) % nk
    before0 = jnp.sum(jnp.where(source < me, first, 0), axis=0, keepdims=True)
    before1 = jnp.sum(jnp.where(source < me, second, 0), axis=0, keepdims=True)
    total0 = jnp.sum(first, axis=0, keepdims=True)
    for j, offset in enumerate((before0, total0 + before1)):
        mine = jnp.sum(jnp.where(ids_col[:, j:j + 1] == lanes, offset, 0), axis=1, keepdims=True)
        wcol[:, j:j + 1] = jnp.where(mine + rcol[:, 2 + j:3 + j] < capacity, turned[:, 2 + j:3 + j], 0.0)

    acc0[...] = jnp.zeros_like(acc0)
    acc1[...] = jnp.zeros_like(acc1)
    xs[dense:wire, :] = jnp.zeros((wire - dense, model), BF16)

    def combine(g, carry):
        wait_group(obuf, retbuf, r_send, r_recv, g, True)
        from_wire(retbuf, g, xs)
        cols = iota((tokens, wire), 1)
        for j, acc in enumerate((acc0, acc1)):
            want = rcol[:, j:j + 1] - g * dense
            pick = ones((want == cols) & (cols < dense))
            for b in range(4):
                part = slice(b * step, (b + 1) * step)
                acc[:, part] += jnp.dot(pick, xs[:, part], preferred_element_type=F32)
        return carry
    lax.fori_loop(0, ng, combine, 0)
    out[...] = (x[...].astype(F32) + wcol[:, 0:1] * acc0[...] + wcol[:, 1:2] * acc1[...]).astype(BF16)

    def drain(g, carry):
        wait_group(outbuf, inbuf, d_send, d_recv, g, False)
        wait_group(obuf, retbuf, r_send, r_recv, g, False)
        return carry
    lax.fori_loop(0, ng, drain, 0)


def torus(n):
    return (4, 4, 4, 2) if n == 128 else (2, n // 4, 1, 2)


def solution(mesh):
    n = mesh.shape["expert"]
    row_spec = P(("data", "expert"), None)
    weight_spec = P("expert", None, None)
    dims = torus(n)

    def device_step(token_rows, expert_ids, gate_weights, w_in, w_out):
        tokens, model = token_rows.shape
        hidden = w_in.shape[2]
        nc, ng = dims[0] * dims[1], dims[2] * dims[3]
        wire, dense = nc * WIRE_ROWS, nc * SLOTS
        width = SLOTS * model // WIRE_ROWS
        capacity = n * (tokens * 2 // n)
        vmem = pl.BlockSpec(memory_space=pltpu.VMEM)
        hbm = pl.BlockSpec(memory_space=pl.ANY)
        dma = pltpu.SemaphoreType.DMA
        return pl.pallas_call(
            functools.partial(moe_kernel, dims, capacity),
            out_shape=jax.ShapeDtypeStruct((tokens, model), BF16),
            in_specs=[vmem, vmem, vmem, hbm, hbm],
            out_specs=vmem,
            scratch_shapes=[
                pltpu.VMEM((ng * wire, width), BF16),
                pltpu.VMEM((ng * wire, width), BF16),
                pltpu.VMEM((ng * wire, width), BF16),
                pltpu.VMEM((ng * wire, width), BF16),
                pltpu.VMEM((n, 1, n), I32),
                pltpu.VMEM((model, hidden), BF16),
                pltpu.VMEM((hidden, model), BF16),
                pltpu.VMEM((wire, width), BF16),
                pltpu.VMEM((wire, model), BF16),
                pltpu.VMEM((dense, hidden), BF16),
                pltpu.VMEM((tokens, model), F32),
                pltpu.VMEM((tokens, model), F32),
                pltpu.VMEM((wire, wire), BF16),
                pltpu.VMEM((wire, wire), BF16),
                pltpu.VMEM((2, tokens), I32),
                pltpu.VMEM((tokens, 4), I32),
                pltpu.VMEM((tokens, 2), F32),
                pltpu.VMEM((8, tokens), F32),
                pltpu.VMEM((tokens, 8), F32),
                dma((2,)), dma((1,)), dma((1,)), dma((ng,)), dma((ng,)), dma((ng,)), dma((ng,)),
            ],
            compiler_params=pltpu.CompilerParams(has_side_effects=True, collective_id=0, vmem_limit_bytes=60 * 1024 * 1024),
        )(expert_ids.T, gate_weights.T, token_rows, w_in, w_out)

    return jax.shard_map(device_step, mesh=mesh, in_specs=(row_spec, row_spec, row_spec, weight_spec, weight_spec), out_specs=row_spec, check_vma=False)
```

```python
import functools

import jax
import jax.numpy as jnp
from jax import lax
from jax.experimental import pallas as pl
from jax.experimental.pallas import tpu as pltpu
from jax.sharding import PartitionSpec as P

SLOTS = 14
WIRE_ROWS = 16
BF16 = jnp.bfloat16
F32 = jnp.float32
I32 = jnp.int32
XORDER = {4: (1, 3, 2, 0), 2: (1, 0)}


def moe_kernel(dims, capacity, ids_row, gates_row, x, win_hbm, wout_hbm, out,
               outbuf, inbuf, obuf, retbuf, cbuf, win, wout, st, xs, hs, acc0, acc1, tmat, tinv, rrow, rcol, wcol, flat, turned,
               w_sem, c_send, c_recv, d_send, d_recv, r_send, r_recv):
    nz, ny, nx, nk = dims
    n = nz * ny * nx * nk
    nc, ng = nz * ny, nx * nk
    tokens, model = x.shape
    hidden = win.shape[1]
    dense = SLOTS * nc
    wire = WIRE_ROWS * nc
    half, quarter, eighth = model // 2, model // 4, model // 8
    width = SLOTS * model // WIRE_ROWS
    me = lax.axis_index("expert")
    mk = lax.rem(me, nk)
    mx = lax.rem(lax.div(me, nk), nx)
    my = lax.rem(lax.div(me, nk * nx), ny)
    mz = lax.div(me, nk * nx * ny)

    half_z, half_y = nz // 2, ny // 2
    turn = XORDER[nx]

    def each_peer(g, sign, act):
        u, rk = lax.div(g, nk), lax.rem(g, nk)
        core = mk if sign > 0 else lax.rem(mk + rk, nk)
        base = lax.rem(mk + rk, nk)
        parts = {}
        for c in range(nc):
            i, dx = c // nx, turn[c % nx]
            mirror = -1 if 2 * dx > nx else 1
            if (i, mirror) not in parts:
                dz = lax.rem(nz + mirror * i + core * half_z, nz)
                dy = lax.rem(2 * ny + mirror * (u + i) + core * half_y, ny)
                z = lax.rem(mz + nz + sign * dz, nz)
                y = lax.rem(my + ny + sign * dy, ny)
                parts[i, mirror] = (z * ny + y) * (nx * nk) + base
            device = parts[i, mirror] + lax.rem(mx + nx + sign * dx, nx) * nk
            if dx == 0:
                @pl.when(device != me)
                def _():
                    act(c, device)
            else:
                act(c, device)
    own = (mk * half_z) * nx + turn.index(0)
    own_rows = pl.ds(pl.multiple_of(own * WIRE_ROWS, WIRE_ROWS), WIRE_ROWS)

    def start_group(src, dst, ssem, rsem, g, sign):
        def act(c, device):
            rows = pl.ds(pl.multiple_of(g * wire + c * WIRE_ROWS, WIRE_ROWS), WIRE_ROWS)
            pltpu.make_async_remote_copy(src_ref=src.at[rows], dst_ref=dst.at[rows], send_sem=ssem.at[g], recv_sem=rsem.at[g],
                                         device_id={"expert": device}, device_id_type=pl.DeviceIdType.MESH).start()
        each_peer(g, sign, act)

    def wait_group(src, dst, ssem, rsem, g, recv):
        def wait(first, count):
            rows = pl.ds(pl.multiple_of(first, WIRE_ROWS), count)
            copy = pltpu.make_async_remote_copy(src_ref=src.at[rows], dst_ref=dst.at[rows], send_sem=ssem.at[g], recv_sem=rsem.at[g],
                                                device_id={"expert": me}, device_id_type=pl.DeviceIdType.MESH)
            copy.wait_recv() if recv else copy.wait_send()

        @pl.when(g == 0)
        def _():
            wait(WIRE_ROWS, wire - WIRE_ROWS)

        @pl.when(g > 0)
        def _():
            wait(g * wire, wire)

    def row_of(ids, slot):
        dz = (ids // (nk * nx * ny) + nz - mz + mk * half_z) % nz
        dy = ((ids // (nk * nx)) % ny + ny - my + mk * half_y) % ny
        dx = ((ids // nk) % nx + nx - mx) % nx
        dk = (ids % nk + nk - mk) % nk
        flip = 2 * dx > nx
        i = jnp.where(flip, (nz - dz) % nz, dz)
        u = (jnp.where(flip, (ny - dy) % ny, dy) + ny - i) % ny
        q = sum(jnp.where(dx == d, p, 0) for p, d in enumerate(turn))
        return (u * nk + dk) * dense + slot * nc + i * nx + q

    def iota(shape, dim):
        return lax.broadcasted_iota(I32, shape, dim)

    def ones(mask):
        return jnp.where(mask, jnp.float32(1.0), jnp.float32(0.0)).astype(BF16)

    barrier = pltpu.get_barrier_semaphore()

    def hello(g, carry):
        def act(c, device):
            pl.semaphore_signal(barrier, inc=1, device_id={"expert": device}, device_id_type=pl.DeviceIdType.MESH)
        each_peer(g, 1, act)
        return carry
    lax.fori_loop(0, ng, hello, 0)

    weights_in = pltpu.make_async_copy(win_hbm.at[0], win, w_sem.at[0])
    weights_out = pltpu.make_async_copy(wout_hbm.at[0], wout, w_sem.at[1])
    weights_in.start()
    weights_out.start()

    flat[0:2, :] = ids_row[...].astype(F32)
    flat[2:4, :] = gates_row[...]
    flat[4:8, :] = jnp.zeros((4, tokens), F32)
    turned[...] = flat[...].T
    ids_col = turned[:, 0:2].astype(I32)

    earlier = iota((tokens, tokens), 0) < iota((tokens, tokens), 1)
    row_ids = [ids_row[j:j + 1, :] for j in range(2)]

    def lane_rank(j, other, mask):
        same = ids_col[:, j:j + 1] == row_ids[other]
        if mask:
            same = same & earlier
        return jnp.sum(jnp.where(same, 1, 0).astype(I32), axis=0, keepdims=True)
    rrow[0:1, :] = row_of(row_ids[0], lane_rank(0, 0, True))
    rrow[1:2, :] = row_of(row_ids[1], lane_rank(1, 1, True) + lane_rank(0, 1, False))

    swap = (iota((wire, wire), 0) % WIRE_ROWS) * nc + iota((wire, wire), 0) // WIRE_ROWS
    tmat[...] = ones(swap == iota((wire, wire), 1))
    swap = (iota((wire, wire), 1) % WIRE_ROWS) * nc + iota((wire, wire), 1) // WIRE_ROWS
    tinv[...] = ones(swap == iota((wire, wire), 0))

    step = quarter

    def stack(b, block):
        h, r = (b * quarter) // half, (b * quarter) % half
        st[h * 8 * nc:(h + 1) * 8 * nc, r:r + quarter] = block[:8 * nc]
        st[b * 4 * nc:(b + 1) * 4 * nc, half:half + quarter] = block[8 * nc:12 * nc]
        for o in range(2):
            st[(2 * b + o) * 2 * nc:(2 * b + o + 1) * 2 * nc, half + quarter:width] = block[12 * nc:, o * eighth:(o + 1) * eighth]

    def to_wire(buf, g):
        rows = pl.ds(pl.multiple_of(g * wire, WIRE_ROWS), wire)
        for lo, hi in ((0, quarter), (quarter, half), (half, half + quarter), (half + quarter, width)):
            buf[rows, lo:hi] = jnp.dot(tmat[...], st[:, lo:hi], preferred_element_type=F32).astype(BF16)

    def from_wire(buf, g, dst):
        rows = pl.ds(pl.multiple_of(g * wire, WIRE_ROWS), wire)
        for r in (0, quarter):
            part = jnp.dot(tinv[...], buf[rows, r:r + quarter], preferred_element_type=F32).astype(BF16)
            dst[0:8 * nc, r:r + quarter] = part[:8 * nc]
            dst[0:8 * nc, half + r:half + r + quarter] = part[8 * nc:]
        part = jnp.dot(tinv[...], buf[rows, half:half + quarter], preferred_element_type=F32).astype(BF16)
        for q in range(4):
            dst[8 * nc:12 * nc, q * quarter:(q + 1) * quarter] = part[q * 4 * nc:(q + 1) * 4 * nc]
        part = jnp.dot(tinv[...], buf[rows, half + quarter:width], preferred_element_type=F32).astype(BF16)
        for o in range(8):
            dst[12 * nc:dense, o * eighth:(o + 1) * eighth] = part[o * 2 * nc:(o + 1) * 2 * nc]

    def build(g, carry):
        rows = iota((dense, tokens), 0) + g * dense
        pick = ones((rows == rrow[0:1, :]) | (rows == rrow[1:2, :]))
        for b in range(4):
            block = jnp.dot(pick, x[:, b * step:(b + 1) * step], preferred_element_type=F32).astype(BF16)
            stack(b, block)
        to_wire(outbuf, g)
        return carry
    lax.fori_loop(0, ng, build, 0)

    lanes = iota((tokens, n), 1)
    count = [jnp.sum(jnp.where(ids_col[:, j:j + 1] == lanes, 1, 0).astype(I32), axis=0, keepdims=True) for j in range(2)]
    cbuf[own] = count[0] + count[1] * 65536

    pl.semaphore_wait(barrier, n - 1)

    def dispatch(g, carry):
        start_group(outbuf, inbuf, d_send, d_recv, g, 1)
        return carry
    lax.fori_loop(0, ng, dispatch, 0)

    def send_counts(g, carry):
        def act(c, device):
            pltpu.make_async_remote_copy(src_ref=cbuf.at[own], dst_ref=cbuf.at[g * nc + c], send_sem=c_send.at[0], recv_sem=c_recv.at[0],
                                         device_id={"expert": device}, device_id_type=pl.DeviceIdType.MESH).start()
        each_peer(g, 1, act)
        return carry
    lax.fori_loop(0, ng, send_counts, 0)
    inbuf[own_rows, :] = outbuf[own_rows, :]

    later = iota((tokens, tokens), 1) < iota((tokens, tokens), 0)

    def sub_rank(j, other, mask):
        same = ids_col[:, other:other + 1] == row_ids[j]
        if mask:
            same = same & later
        return jnp.sum(jnp.where(same, 1, 0).astype(I32), axis=1, keepdims=True)
    rank0 = sub_rank(0, 0, True)
    rank1 = sub_rank(1, 1, True)
    rcol[:, 0:1] = row_of(ids_col[:, 0:1], rank0)
    rcol[:, 1:2] = row_of(ids_col[:, 1:2], rank1 + sub_rank(0, 1, False))
    rcol[:, 2:3] = rank0
    rcol[:, 3:4] = rank1

    weights_in.wait()
    weights_out.wait()

    def expert(g, carry):
        wait_group(outbuf, inbuf, d_send, d_recv, g, True)
        from_wire(inbuf, g, xs)
        for b in range(4):
            cols = slice(b * hidden // 4, (b + 1) * hidden // 4)
            pre = jnp.dot(xs[0:dense, :], win[:, cols], preferred_element_type=F32)
            hs[:, cols] = jax.nn.gelu(pre).astype(BF16)
        for b in range(4):
            block = jnp.dot(hs[...], wout[:, b * step:(b + 1) * step], preferred_element_type=F32).astype(BF16)
            stack(b, block)
        to_wire(obuf, g)
        start_group(obuf, retbuf, r_send, r_recv, g, -1)
        return carry
    lax.fori_loop(0, ng, expert, 0)
    retbuf[own_rows, :] = obuf[own_rows, :]

    pltpu.make_async_remote_copy(src_ref=cbuf.at[pl.ds(1, n - 1)], dst_ref=cbuf.at[pl.ds(1, n - 1)], send_sem=c_send.at[0], recv_sem=c_recv.at[0],
                                 device_id={"expert": me}, device_id_type=pl.DeviceIdType.MESH).wait()

    packed = cbuf[...].reshape(n, n)
    second = packed // 65536
    first = packed - second * 65536
    slot = iota((n, n), 0)
    g, c = slot // nc, slot % nc
    u, rk, i = g // nk, g % nk, c // nx
    dx = sum(jnp.where(c % nx == p, d, 0) for p, d in enumerate(turn))
    mirror = jnp.where(2 * dx > nx, -1, 1)
    core = (mk + rk) % nk
    dz = (nz + mirror * i + core * half_z) % nz
    dy = (2 * ny + mirror * (u + i) + core * half_y) % ny
    source = (((mz + nz - dz) % nz * ny + (my + ny - dy) % ny) * nx + (mx + nx - dx) % nx) * nk + core
    before0 = jnp.sum(jnp.where(source < me, first, 0), axis=0, keepdims=True)
    before1 = jnp.sum(jnp.where(source < me, second, 0), axis=0, keepdims=True)
    total0 = jnp.sum(first, axis=0, keepdims=True)
    for j, offset in enumerate((before0, total0 + before1)):
        mine = jnp.sum(jnp.where(ids_col[:, j:j + 1] == lanes, offset, 0), axis=1, keepdims=True)
        wcol[:, j:j + 1] = jnp.where(mine + rcol[:, 2 + j:3 + j] < capacity, turned[:, 2 + j:3 + j], 0.0)

    acc0[...] = jnp.zeros_like(acc0)
    acc1[...] = jnp.zeros_like(acc1)
    xs[dense:wire, :] = jnp.zeros((wire - dense, model), BF16)

    def combine(g, carry):
        wait_group(obuf, retbuf, r_send, r_recv, g, True)
        from_wire(retbuf, g, xs)
        cols = iota((tokens, wire), 1)
        for j, acc in enumerate((acc0, acc1)):
            want = rcol[:, j:j + 1] - g * dense
            pick = ones((want == cols) & (cols < dense))
            for b in range(4):
                part = slice(b * step, (b + 1) * step)
                acc[:, part] += jnp.dot(pick, xs[:, part], preferred_element_type=F32)
        return carry
    lax.fori_loop(0, ng, combine, 0)
    out[...] = (x[...].astype(F32) + wcol[:, 0:1] * acc0[...] + wcol[:, 1:2] * acc1[...]).astype(BF16)

    def drain(g, carry):
        wait_group(outbuf, inbuf, d_send, d_recv, g, False)
        wait_group(obuf, retbuf, r_send, r_recv, g, False)
        return carry
    lax.fori_loop(0, ng, drain, 0)


def torus(n):
    return (4, 4, 4, 2) if n == 128 else (2, 2, 2, 2)


def solution(mesh):
    n = mesh.shape["expert"]
    row_spec = P(("data", "expert"), None)
    weight_spec = P("expert", None, None)
    dims = torus(n)

    def device_step(token_rows, expert_ids, gate_weights, w_in, w_out):
        tokens, model = token_rows.shape
        hidden = w_in.shape[2]
        nc, ng = dims[0] * dims[1], dims[2] * dims[3]
        wire, dense = nc * WIRE_ROWS, nc * SLOTS
        width = SLOTS * model // WIRE_ROWS
        capacity = n * (tokens * 2 // n)
        vmem = pl.BlockSpec(memory_space=pltpu.VMEM)
        hbm = pl.BlockSpec(memory_space=pl.ANY)
        dma = pltpu.SemaphoreType.DMA
        return pl.pallas_call(
            functools.partial(moe_kernel, dims, capacity),
            out_shape=jax.ShapeDtypeStruct((tokens, model), BF16),
            in_specs=[vmem, vmem, vmem, hbm, hbm],
            out_specs=vmem,
            scratch_shapes=[
                pltpu.VMEM((ng * wire, width), BF16),
                pltpu.VMEM((ng * wire, width), BF16),
                pltpu.VMEM((ng * wire, width), BF16),
                pltpu.VMEM((ng * wire, width), BF16),
                pltpu.VMEM((n, 1, n), I32),
                pltpu.VMEM((model, hidden), BF16),
                pltpu.VMEM((hidden, model), BF16),
                pltpu.VMEM((wire, width), BF16),
                pltpu.VMEM((wire, model), BF16),
                pltpu.VMEM((dense, hidden), BF16),
                pltpu.VMEM((tokens, model), F32),
                pltpu.VMEM((tokens, model), F32),
                pltpu.VMEM((wire, wire), BF16),
                pltpu.VMEM((wire, wire), BF16),
                pltpu.VMEM((2, tokens), I32),
                pltpu.VMEM((tokens, 4), I32),
                pltpu.VMEM((tokens, 2), F32),
                pltpu.VMEM((8, tokens), F32),
                pltpu.VMEM((tokens, 8), F32),
                dma((2,)), dma((1,)), dma((1,)), dma((ng,)), dma((ng,)), dma((ng,)), dma((ng,)),
            ],
            compiler_params=pltpu.CompilerParams(has_side_effects=True, collective_id=0, vmem_limit_bytes=60 * 1024 * 1024),
        )(expert_ids.T, gate_weights.T, token_rows, w_in, w_out)

    return jax.shard_map(device_step, mesh=mesh, in_specs=(row_spec, row_spec, row_spec, weight_spec, weight_spec), out_specs=row_spec, check_vma=False)
```

```python
import functools

import jax
import jax.numpy as jnp
from jax import lax
from jax.experimental import pallas as pl
from jax.experimental.pallas import tpu as pltpu
from jax.sharding import PartitionSpec as P

SLOTS = 14
WIRE_ROWS = 16
BF16 = jnp.bfloat16
F32 = jnp.float32
I32 = jnp.int32
VMEM_LIMIT = 60 * 1024 * 1024
XORDER = {4: (1, 3, 2, 0), 2: (1, 0)}


def moe_kernel(dims, capacity, ids_hbm, gates_hbm, x_hbm, win_hbm, wout_hbm, out,
               ids_row, gates_row, x, outbuf, inbuf, obuf, retbuf, cbuf, win, wout, st, xs, hs, acc0, acc1, tmat, tinv, rrow, rcol, wcol, flat, turned,
               w_sem, c_send, c_recv, d_send, d_recv, r_send, r_recv):
    nz, ny, nx, nk = dims
    n = nz * ny * nx * nk
    nc, ng = nz * ny, nx * nk
    tokens, model = x_hbm.shape
    hidden = win.shape[1]
    dense = SLOTS * nc
    wire = WIRE_ROWS * nc
    half, quarter, eighth = model // 2, model // 4, model // 8
    width = SLOTS * model // WIRE_ROWS
    me = lax.axis_index("expert")
    mk = lax.rem(me, nk)
    mx = lax.rem(lax.div(me, nk), nx)
    my = lax.rem(lax.div(me, nk * nx), ny)
    mz = lax.div(me, nk * nx * ny)

    half_z, half_y = nz // 2, ny // 2
    turn = XORDER[nx]

    def each_peer(g, sign, act):
        u, rk = lax.div(g, nk), lax.rem(g, nk)
        core = mk if sign > 0 else lax.rem(mk + rk, nk)
        base = lax.rem(mk + rk, nk)
        parts = {}
        for c in range(nc):
            i, dx = c // nx, turn[c % nx]
            mirror = -1 if 2 * dx > nx else 1
            if (i, mirror) not in parts:
                dz = lax.rem(nz + mirror * i + core * half_z, nz)
                dy = lax.rem(2 * ny + mirror * (u + i) + core * half_y, ny)
                z = lax.rem(mz + nz + sign * dz, nz)
                y = lax.rem(my + ny + sign * dy, ny)
                parts[i, mirror] = (z * ny + y) * (nx * nk) + base
            device = parts[i, mirror] + lax.rem(mx + nx + sign * dx, nx) * nk
            if dx == 0:
                @pl.when(device != me)
                def _():
                    act(c, device)
            else:
                act(c, device)
    own = (mk * half_z) * nx + turn.index(0)
    own_rows = pl.ds(pl.multiple_of(own * WIRE_ROWS, WIRE_ROWS), WIRE_ROWS)

    def start_group(src, dst, ssem, rsem, g, sign):
        def act(c, device):
            rows = pl.ds(pl.multiple_of(g * wire + c * WIRE_ROWS, WIRE_ROWS), WIRE_ROWS)
            pltpu.make_async_remote_copy(src_ref=src.at[rows], dst_ref=dst.at[rows], send_sem=ssem.at[g], recv_sem=rsem.at[g],
                                         device_id={"expert": device}, device_id_type=pl.DeviceIdType.MESH).start()
        each_peer(g, sign, act)

    def wait_group(src, dst, ssem, rsem, g, recv):
        def wait(first, count):
            rows = pl.ds(pl.multiple_of(first, WIRE_ROWS), count)
            copy = pltpu.make_async_remote_copy(src_ref=src.at[rows], dst_ref=dst.at[rows], send_sem=ssem.at[g], recv_sem=rsem.at[g],
                                                device_id={"expert": me}, device_id_type=pl.DeviceIdType.MESH)
            copy.wait_recv() if recv else copy.wait_send()

        @pl.when(g == 0)
        def _():
            wait(WIRE_ROWS, wire - WIRE_ROWS)

        @pl.when(g > 0)
        def _():
            wait(g * wire, wire)

    def row_of(ids, slot):
        dz = (ids // (nk * nx * ny) + nz - mz + mk * half_z) % nz
        dy = ((ids // (nk * nx)) % ny + ny - my + mk * half_y) % ny
        dx = ((ids // nk) % nx + nx - mx) % nx
        dk = (ids % nk + nk - mk) % nk
        flip = 2 * dx > nx
        i = jnp.where(flip, (nz - dz) % nz, dz)
        u = (jnp.where(flip, (ny - dy) % ny, dy) + ny - i) % ny
        q = sum(jnp.where(dx == d, p, 0) for p, d in enumerate(turn))
        return (u * nk + dk) * dense + slot * nc + i * nx + q

    def iota(shape, dim):
        return lax.broadcasted_iota(I32, shape, dim)

    def ones(mask):
        return jnp.where(mask, jnp.float32(1.0), jnp.float32(0.0)).astype(BF16)

    fetch = [pltpu.make_async_copy(src, dst, w_sem.at[i]) for i, (src, dst) in enumerate((
        (ids_hbm, ids_row), (gates_hbm, gates_row), (x_hbm, x), (win_hbm.at[0], win), (wout_hbm.at[0], wout)))]
    for copy in fetch:
        copy.start()

    barrier = pltpu.get_barrier_semaphore()

    def hello(i, carry):
        pl.semaphore_signal(barrier, inc=1, device_id={"expert": lax.rem(me + i, n)}, device_id_type=pl.DeviceIdType.MESH)
        return carry
    lax.fori_loop(1, n, hello, 0, unroll=4)
    fetch[0].wait()
    fetch[1].wait()

    flat[0:2, :] = ids_row[...].astype(F32)
    flat[2:4, :] = gates_row[...]
    flat[4:8, :] = jnp.zeros((4, tokens), F32)
    turned[...] = flat[...].T
    ids_col = turned[:, 0:2].astype(I32)

    earlier = iota((tokens, tokens), 0) < iota((tokens, tokens), 1)
    row_ids = [ids_row[j:j + 1, :] for j in range(2)]

    def lane_rank(j, other, mask):
        same = ids_col[:, j:j + 1] == row_ids[other]
        if mask:
            same = same & earlier
        return jnp.sum(jnp.where(same, 1, 0).astype(I32), axis=0, keepdims=True)
    rrow[0:1, :] = row_of(row_ids[0], lane_rank(0, 0, True))
    rrow[1:2, :] = row_of(row_ids[1], lane_rank(1, 1, True) + lane_rank(0, 1, False))

    swap = (iota((wire, wire), 0) % WIRE_ROWS) * nc + iota((wire, wire), 0) // WIRE_ROWS
    tmat[...] = ones(swap == iota((wire, wire), 1))
    swap = (iota((wire, wire), 1) % WIRE_ROWS) * nc + iota((wire, wire), 1) // WIRE_ROWS
    tinv[...] = ones(swap == iota((wire, wire), 0))

    step = quarter

    def stack(b, block):
        h, r = (b * quarter) // half, (b * quarter) % half
        st[h * 8 * nc:(h + 1) * 8 * nc, r:r + quarter] = block[:8 * nc]
        st[b * 4 * nc:(b + 1) * 4 * nc, half:half + quarter] = block[8 * nc:12 * nc]
        for o in range(2):
            st[(2 * b + o) * 2 * nc:(2 * b + o + 1) * 2 * nc, half + quarter:width] = block[12 * nc:, o * eighth:(o + 1) * eighth]

    def to_wire(buf, g):
        rows = pl.ds(pl.multiple_of(g * wire, WIRE_ROWS), wire)
        for lo, hi in ((0, quarter), (quarter, half), (half, half + quarter), (half + quarter, width)):
            buf[rows, lo:hi] = jnp.dot(tmat[...], st[:, lo:hi], preferred_element_type=F32).astype(BF16)

    def from_wire(buf, g, dst):
        rows = pl.ds(pl.multiple_of(g * wire, WIRE_ROWS), wire)
        for r in (0, quarter):
            part = jnp.dot(tinv[...], buf[rows, r:r + quarter], preferred_element_type=F32).astype(BF16)
            dst[0:8 * nc, r:r + quarter] = part[:8 * nc]
            dst[0:8 * nc, half + r:half + r + quarter] = part[8 * nc:]
        part = jnp.dot(tinv[...], buf[rows, half:half + quarter], preferred_element_type=F32).astype(BF16)
        for q in range(4):
            dst[8 * nc:12 * nc, q * quarter:(q + 1) * quarter] = part[q * 4 * nc:(q + 1) * 4 * nc]
        part = jnp.dot(tinv[...], buf[rows, half + quarter:width], preferred_element_type=F32).astype(BF16)
        for o in range(8):
            dst[12 * nc:dense, o * eighth:(o + 1) * eighth] = part[o * 2 * nc:(o + 1) * 2 * nc]

    def build(g, carry):
        rows = iota((dense, tokens), 0) + g * dense
        pick = ones((rows == rrow[0:1, :]) | (rows == rrow[1:2, :]))
        for b in range(4):
            block = jnp.dot(pick, x[:, b * step:(b + 1) * step], preferred_element_type=F32).astype(BF16)
            stack(b, block)
        to_wire(outbuf, g)
        return carry
    fetch[2].wait()
    lax.fori_loop(0, ng // 2, build, 0)

    lanes = iota((tokens, n), 1)
    count = [jnp.sum(jnp.where(ids_col[:, j:j + 1] == lanes, 1, 0).astype(I32), axis=0, keepdims=True) for j in range(2)]
    cbuf[own] = count[0] + count[1] * 65536

    pl.semaphore_wait(barrier, n - 1)

    def dispatch(g, carry):
        start_group(outbuf, inbuf, d_send, d_recv, g, 1)
        return carry
    lax.fori_loop(0, ng // 2, dispatch, 0)

    def build_dispatch(g, carry):
        return dispatch(g, build(g, carry))
    lax.fori_loop(ng // 2, ng, build_dispatch, 0)

    def send_counts(g, carry):
        def act(c, device):
            pltpu.make_async_remote_copy(src_ref=cbuf.at[own], dst_ref=cbuf.at[g * nc + c], send_sem=c_send.at[0], recv_sem=c_recv.at[0],
                                         device_id={"expert": device}, device_id_type=pl.DeviceIdType.MESH).start()
        each_peer(g, 1, act)
        return carry
    lax.fori_loop(0, ng, send_counts, 0)
    inbuf[own_rows, :] = outbuf[own_rows, :]

    later = iota((tokens, tokens), 1) < iota((tokens, tokens), 0)

    def sub_rank(j, other, mask):
        same = ids_col[:, other:other + 1] == row_ids[j]
        if mask:
            same = same & later
        return jnp.sum(jnp.where(same, 1, 0).astype(I32), axis=1, keepdims=True)
    rank0 = sub_rank(0, 0, True)
    rank1 = sub_rank(1, 1, True)
    rcol[:, 0:1] = row_of(ids_col[:, 0:1], rank0)
    rcol[:, 1:2] = row_of(ids_col[:, 1:2], rank1 + sub_rank(0, 1, False))
    rcol[:, 2:3] = rank0
    rcol[:, 3:4] = rank1

    fetch[3].wait()
    fetch[4].wait()

    def expert(g, carry):
        wait_group(outbuf, inbuf, d_send, d_recv, g, True)
        from_wire(inbuf, g, xs)
        for b in range(4):
            cols = slice(b * hidden // 4, (b + 1) * hidden // 4)
            pre = jnp.dot(xs[0:dense, :], win[:, cols], preferred_element_type=F32)
            hs[:, cols] = jax.nn.gelu(pre).astype(BF16)
        for b in range(4):
            block = jnp.dot(hs[...], wout[:, b * step:(b + 1) * step], preferred_element_type=F32).astype(BF16)
            stack(b, block)
        to_wire(obuf, g)
        start_group(obuf, retbuf, r_send, r_recv, g, -1)
        return carry
    lax.fori_loop(0, ng, expert, 0)
    retbuf[own_rows, :] = obuf[own_rows, :]

    pltpu.make_async_remote_copy(src_ref=cbuf.at[pl.ds(1, n - 1)], dst_ref=cbuf.at[pl.ds(1, n - 1)], send_sem=c_send.at[0], recv_sem=c_recv.at[0],
                                 device_id={"expert": me}, device_id_type=pl.DeviceIdType.MESH).wait()

    packed = cbuf[...].reshape(n, n)
    second = packed // 65536
    first = packed - second * 65536
    slot = iota((n, n), 0)
    g, c = slot // nc, slot % nc
    u, rk, i = g // nk, g % nk, c // nx
    dx = sum(jnp.where(c % nx == p, d, 0) for p, d in enumerate(turn))
    mirror = jnp.where(2 * dx > nx, -1, 1)
    core = (mk + rk) % nk
    dz = (nz + mirror * i + core * half_z) % nz
    dy = (2 * ny + mirror * (u + i) + core * half_y) % ny
    source = (((mz + nz - dz) % nz * ny + (my + ny - dy) % ny) * nx + (mx + nx - dx) % nx) * nk + core
    before0 = jnp.sum(jnp.where(source < me, first, 0), axis=0, keepdims=True)
    before1 = jnp.sum(jnp.where(source < me, second, 0), axis=0, keepdims=True)
    total0 = jnp.sum(first, axis=0, keepdims=True)
    for j, offset in enumerate((before0, total0 + before1)):
        mine = jnp.sum(jnp.where(ids_col[:, j:j + 1] == lanes, offset, 0), axis=1, keepdims=True)
        wcol[:, j:j + 1] = jnp.where(mine + rcol[:, 2 + j:3 + j] < capacity, turned[:, 2 + j:3 + j], 0.0)

    acc0[...] = jnp.zeros_like(acc0)
    acc1[...] = jnp.zeros_like(acc1)
    xs[dense:wire, :] = jnp.zeros((wire - dense, model), BF16)

    def picks(g):
        cols = iota((tokens, wire), 1)
        wants = [rcol[:, j:j + 1] - g * dense for j in range(2)]
        return [ones((want == cols) & (cols < dense)) for want in wants]

    def combine(g, carry):
        wait_group(obuf, retbuf, r_send, r_recv, g, True)
        from_wire(retbuf, g, xs)
        for pick, acc in zip(picks(g), (acc0, acc1)):
            for b in range(4):
                part = slice(b * step, (b + 1) * step)
                acc[:, part] += jnp.dot(pick, xs[:, part], preferred_element_type=F32)
        return carry
    lax.fori_loop(0, ng - 1, combine, 0)

    last = ng - 1
    wait_group(obuf, retbuf, r_send, r_recv, last, True)
    from_wire(retbuf, last, xs)
    pick0, pick1 = picks(last)
    for b in range(4):
        part = slice(b * step, (b + 1) * step)
        first = acc0[:, part] + jnp.dot(pick0, xs[:, part], preferred_element_type=F32)
        second = acc1[:, part] + jnp.dot(pick1, xs[:, part], preferred_element_type=F32)
        out[:, part] = (x[:, part].astype(F32) + wcol[:, 0:1] * first + wcol[:, 1:2] * second).astype(BF16)

    def drain(g, carry):
        wait_group(outbuf, inbuf, d_send, d_recv, g, False)
        wait_group(obuf, retbuf, r_send, r_recv, g, False)
        return carry
    lax.fori_loop(0, ng, drain, 0)


def torus(n):
    return (4, 4, 4, 2) if n == 128 else (2, 2, 2, 2)


def solution(mesh):
    n = mesh.shape["expert"]
    row_spec = P(("data", "expert"), None)
    weight_spec = P("expert", None, None)
    dims = torus(n)

    def device_step(token_rows, expert_ids, gate_weights, w_in, w_out):
        tokens, model = token_rows.shape
        hidden = w_in.shape[2]
        nc, ng = dims[0] * dims[1], dims[2] * dims[3]
        wire, dense = nc * WIRE_ROWS, nc * SLOTS
        width = SLOTS * model // WIRE_ROWS
        capacity = n * (tokens * 2 // n)
        vmem = pl.BlockSpec(memory_space=pltpu.VMEM)
        hbm = pl.BlockSpec(memory_space=pltpu.HBM)
        dma = pltpu.SemaphoreType.DMA
        return pl.pallas_call(
            functools.partial(moe_kernel, dims, capacity),
            out_shape=jax.ShapeDtypeStruct((tokens, model), BF16),
            in_specs=[hbm] * 5,
            out_specs=vmem,
            scratch_shapes=[
                pltpu.VMEM((2, tokens), I32),
                pltpu.VMEM((2, tokens), F32),
                pltpu.VMEM((tokens, model), BF16),
                pltpu.VMEM((ng * wire, width), BF16),
                pltpu.VMEM((ng * wire, width), BF16),
                pltpu.VMEM((ng * wire, width), BF16),
                pltpu.VMEM((ng * wire, width), BF16),
                pltpu.VMEM((n, 1, n), I32),
                pltpu.VMEM((model, hidden), BF16),
                pltpu.VMEM((hidden, model), BF16),
                pltpu.VMEM((wire, width), BF16),
                pltpu.VMEM((wire, model), BF16),
                pltpu.VMEM((dense, hidden), BF16),
                pltpu.VMEM((tokens, model), F32),
                pltpu.VMEM((tokens, model), F32),
                pltpu.VMEM((wire, wire), BF16),
                pltpu.VMEM((wire, wire), BF16),
                pltpu.VMEM((2, tokens), I32),
                pltpu.VMEM((tokens, 4), I32),
                pltpu.VMEM((tokens, 2), F32),
                pltpu.VMEM((8, tokens), F32),
                pltpu.VMEM((tokens, 8), F32),
                dma((5,)), dma((1,)), dma((1,)), dma((ng,)), dma((ng,)), dma((ng,)), dma((ng,)),
            ],
            compiler_params=pltpu.CompilerParams(has_side_effects=True, collective_id=0, vmem_limit_bytes=VMEM_LIMIT),
        )(expert_ids.T, gate_weights.T, token_rows, w_in, w_out)

    return jax.shard_map(device_step, mesh=mesh, in_specs=(row_spec, row_spec, row_spec, weight_spec, weight_spec), out_specs=row_spec, check_vma=False)
```

```python
import functools

import jax
import jax.numpy as jnp
from jax import lax
from jax.experimental import pallas as pl
from jax.experimental.pallas import tpu as pltpu
from jax.sharding import PartitionSpec as P

SLOTS = 14
WIRE_ROWS = 16
BF16 = jnp.bfloat16
F32 = jnp.float32
I32 = jnp.int32
VMEM_LIMIT = 60 * 1024 * 1024
XORDER = {4: (2, 1, 0, 3), 2: (1, 0)}


def moe_kernel(dims, capacity, ids_hbm, gates_hbm, x_hbm, win_hbm, wout_hbm, out,
               ids_row, gates_row, x, outbuf, inbuf, obuf, retbuf, cbuf, win, wout, st, xs, hs, acc0, acc1, total, tmat, tinv, rrow, rcol, wcol, flat, turned,
               w_sem, o_sem, c_send, c_recv, d_send, d_recv, r_send, r_recv):
    nz, ny, nx, nk = dims
    n = nz * ny * nx * nk
    nc, ng = nz * ny, nx * nk
    tokens, model = x_hbm.shape
    hidden = win.shape[1]
    dense = SLOTS * nc
    wire = WIRE_ROWS * nc
    half, quarter, eighth = model // 2, model // 4, model // 8
    width = SLOTS * model // WIRE_ROWS
    me = lax.axis_index("expert")
    mk = lax.rem(me, nk)
    mx = lax.rem(lax.div(me, nk), nx)
    my = lax.rem(lax.div(me, nk * nx), ny)
    mz = lax.div(me, nk * nx * ny)

    half_z, half_y = nz // 2, ny // 2
    turn = XORDER[nx]

    def each_peer(g, sign, act):
        u, rk = lax.div(g, nk), lax.rem(g, nk)
        core = mk if sign > 0 else lax.rem(mk + rk, nk)
        base = lax.rem(mk + rk, nk)
        parts = {}
        for c in range(nc):
            i, dx = c // nx, turn[c % nx]
            mirror = -1 if 2 * dx > nx else 1
            if (i, mirror) not in parts:
                dz = lax.rem(nz + mirror * i + core * half_z, nz)
                dy = lax.rem(2 * ny + mirror * (u + i) + core * half_y, ny)
                z = lax.rem(mz + nz + sign * dz, nz)
                y = lax.rem(my + ny + sign * dy, ny)
                parts[i, mirror] = (z * ny + y) * (nx * nk) + base
            device = parts[i, mirror] + lax.rem(mx + nx + sign * dx, nx) * nk
            if dx == 0:
                @pl.when(device != me)
                def _():
                    act(c, device)
            else:
                act(c, device)
    own = (mk * half_z) * nx + turn.index(0)
    own_rows = pl.ds(pl.multiple_of(own * WIRE_ROWS, WIRE_ROWS), WIRE_ROWS)

    def start_group(src, dst, ssem, rsem, g, sign):
        def act(c, device):
            rows = pl.ds(pl.multiple_of(g * wire + c * WIRE_ROWS, WIRE_ROWS), WIRE_ROWS)
            pltpu.make_async_remote_copy(src_ref=src.at[rows], dst_ref=dst.at[rows], send_sem=ssem.at[g], recv_sem=rsem.at[g],
                                         device_id={"expert": device}, device_id_type=pl.DeviceIdType.MESH).start()
        each_peer(g, sign, act)

    def wait_group(src, dst, ssem, rsem, g, recv):
        def wait(first, count):
            rows = pl.ds(pl.multiple_of(first, WIRE_ROWS), count)
            copy = pltpu.make_async_remote_copy(src_ref=src.at[rows], dst_ref=dst.at[rows], send_sem=ssem.at[g], recv_sem=rsem.at[g],
                                                device_id={"expert": me}, device_id_type=pl.DeviceIdType.MESH)
            copy.wait_recv() if recv else copy.wait_send()

        @pl.when(g == 0)
        def _():
            wait(WIRE_ROWS, wire - WIRE_ROWS)

        @pl.when(g > 0)
        def _():
            wait(g * wire, wire)

    def row_of(ids, slot):
        dz = (ids // (nk * nx * ny) + nz - mz + mk * half_z) % nz
        dy = ((ids // (nk * nx)) % ny + ny - my + mk * half_y) % ny
        dx = ((ids // nk) % nx + nx - mx) % nx
        dk = (ids % nk + nk - mk) % nk
        flip = 2 * dx > nx
        i = jnp.where(flip, (nz - dz) % nz, dz)
        u = (jnp.where(flip, (ny - dy) % ny, dy) + ny - i) % ny
        q = sum(jnp.where(dx == d, p, 0) for p, d in enumerate(turn))
        return (u * nk + dk) * dense + slot * nc + i * nx + q

    def iota(shape, dim):
        return lax.broadcasted_iota(I32, shape, dim)

    def ones(mask):
        return jnp.where(mask, jnp.float32(1.0), jnp.float32(0.0)).astype(BF16)

    fetch = [pltpu.make_async_copy(src, dst, w_sem.at[i]) for i, (src, dst) in enumerate((
        (ids_hbm, ids_row), (gates_hbm, gates_row), (x_hbm, x), (win_hbm.at[0], win), (wout_hbm.at[0], wout)))]
    for copy in fetch:
        copy.start()

    barrier = pltpu.get_barrier_semaphore()

    def hello(i, carry):
        pl.semaphore_signal(barrier, inc=1, device_id={"expert": lax.rem(me + i, n)}, device_id_type=pl.DeviceIdType.MESH)
        return carry
    lax.fori_loop(1, n, hello, 0, unroll=4)
    fetch[0].wait()
    fetch[1].wait()

    flat[0:2, :] = ids_row[...].astype(F32)
    flat[2:4, :] = gates_row[...]
    flat[4:8, :] = jnp.zeros((4, tokens), F32)
    turned[...] = flat[...].T
    ids_col = turned[:, 0:2].astype(I32)

    earlier = iota((tokens, tokens), 0) < iota((tokens, tokens), 1)
    row_ids = [ids_row[j:j + 1, :] for j in range(2)]

    def lane_rank(j, other, mask):
        same = ids_col[:, j:j + 1] == row_ids[other]
        if mask:
            same = same & earlier
        return jnp.sum(jnp.where(same, 1, 0).astype(I32), axis=0, keepdims=True)
    rrow[0:1, :] = row_of(row_ids[0], lane_rank(0, 0, True))
    rrow[1:2, :] = row_of(row_ids[1], lane_rank(1, 1, True) + lane_rank(0, 1, False))

    swap = (iota((wire, wire), 0) % WIRE_ROWS) * nc + iota((wire, wire), 0) // WIRE_ROWS
    tmat[...] = ones(swap == iota((wire, wire), 1))
    swap = (iota((wire, wire), 1) % WIRE_ROWS) * nc + iota((wire, wire), 1) // WIRE_ROWS
    tinv[...] = ones(swap == iota((wire, wire), 0))

    step = quarter

    def stack(b, block):
        h, r = (b * quarter) // half, (b * quarter) % half
        st[h * 8 * nc:(h + 1) * 8 * nc, r:r + quarter] = block[:8 * nc]
        st[b * 4 * nc:(b + 1) * 4 * nc, half:half + quarter] = block[8 * nc:12 * nc]
        for o in range(2):
            st[(2 * b + o) * 2 * nc:(2 * b + o + 1) * 2 * nc, half + quarter:width] = block[12 * nc:, o * eighth:(o + 1) * eighth]

    def to_wire(buf, g):
        rows = pl.ds(pl.multiple_of(g * wire, WIRE_ROWS), wire)
        for lo, hi in ((0, quarter), (quarter, half), (half, half + quarter), (half + quarter, width)):
            buf[rows, lo:hi] = jnp.dot(tmat[...], st[:, lo:hi], preferred_element_type=F32).astype(BF16)

    def from_wire(buf, g, dst):
        rows = pl.ds(pl.multiple_of(g * wire, WIRE_ROWS), wire)
        for r in (0, quarter):
            part = jnp.dot(tinv[...], buf[rows, r:r + quarter], preferred_element_type=F32).astype(BF16)
            dst[0:8 * nc, r:r + quarter] = part[:8 * nc]
            dst[0:8 * nc, half + r:half + r + quarter] = part[8 * nc:]
        part = jnp.dot(tinv[...], buf[rows, half:half + quarter], preferred_element_type=F32).astype(BF16)
        for q in range(4):
            dst[8 * nc:12 * nc, q * quarter:(q + 1) * quarter] = part[q * 4 * nc:(q + 1) * 4 * nc]
        part = jnp.dot(tinv[...], buf[rows, half + quarter:width], preferred_element_type=F32).astype(BF16)
        for o in range(8):
            dst[12 * nc:dense, o * eighth:(o + 1) * eighth] = part[o * 2 * nc:(o + 1) * 2 * nc]

    def build(g, carry):
        rows = iota((dense, tokens), 0) + g * dense
        pick = ones((rows == rrow[0:1, :]) | (rows == rrow[1:2, :]))
        for b in range(4):
            block = jnp.dot(pick, x[:, b * step:(b + 1) * step], preferred_element_type=F32).astype(BF16)
            stack(b, block)
        to_wire(outbuf, g)
        return carry
    fetch[2].wait()
    lax.fori_loop(0, ng // 2, build, 0)

    lanes = iota((tokens, n), 1)
    count = [jnp.sum(jnp.where(ids_col[:, j:j + 1] == lanes, 1, 0).astype(I32), axis=0, keepdims=True) for j in range(2)]
    cbuf[own] = count[0] + count[1] * 65536

    pl.semaphore_wait(barrier, n - 1)

    def dispatch(g, carry):
        start_group(outbuf, inbuf, d_send, d_recv, g, 1)
        return carry
    lax.fori_loop(0, ng // 2, dispatch, 0)

    def build_dispatch(g, carry):
        return dispatch(g, build(g, carry))
    lax.fori_loop(ng // 2, ng, build_dispatch, 0)

    def send_counts(g, carry):
        def act(c, device):
            pltpu.make_async_remote_copy(src_ref=cbuf.at[own], dst_ref=cbuf.at[g * nc + c], send_sem=c_send.at[0], recv_sem=c_recv.at[0],
                                         device_id={"expert": device}, device_id_type=pl.DeviceIdType.MESH).start()
        each_peer(g, 1, act)
        return carry
    lax.fori_loop(0, ng, send_counts, 0)
    inbuf[own_rows, :] = outbuf[own_rows, :]

    later = iota((tokens, tokens), 1) < iota((tokens, tokens), 0)

    def sub_rank(j, other, mask):
        same = ids_col[:, other:other + 1] == row_ids[j]
        if mask:
            same = same & later
        return jnp.sum(jnp.where(same, 1, 0).astype(I32), axis=1, keepdims=True)
    rank0 = sub_rank(0, 0, True)
    rank1 = sub_rank(1, 1, True)
    rcol[:, 0:1] = row_of(ids_col[:, 0:1], rank0)
    rcol[:, 1:2] = row_of(ids_col[:, 1:2], rank1 + sub_rank(0, 1, False))
    rcol[:, 2:3] = rank0
    rcol[:, 3:4] = rank1

    fetch[3].wait()
    fetch[4].wait()

    def expert(g, carry):
        wait_group(outbuf, inbuf, d_send, d_recv, g, True)
        from_wire(inbuf, g, xs)
        for b in range(4):
            cols = slice(b * hidden // 4, (b + 1) * hidden // 4)
            pre = jnp.dot(xs[0:dense, :], win[:, cols], preferred_element_type=F32)
            hs[:, cols] = jax.nn.gelu(pre).astype(BF16)
        for b in range(4):
            block = jnp.dot(hs[...], wout[:, b * step:(b + 1) * step], preferred_element_type=F32).astype(BF16)
            stack(b, block)
        to_wire(obuf, g)
        start_group(obuf, retbuf, r_send, r_recv, g, -1)
        return carry
    lax.fori_loop(0, ng, expert, 0)
    retbuf[own_rows, :] = obuf[own_rows, :]

    pltpu.make_async_remote_copy(src_ref=cbuf.at[pl.ds(1, n - 1)], dst_ref=cbuf.at[pl.ds(1, n - 1)], send_sem=c_send.at[0], recv_sem=c_recv.at[0],
                                 device_id={"expert": me}, device_id_type=pl.DeviceIdType.MESH).wait()

    packed = cbuf[...].reshape(n, n)
    second = packed // 65536
    first = packed - second * 65536
    slot = iota((n, n), 0)
    g, c = slot // nc, slot % nc
    u, rk, i = g // nk, g % nk, c // nx
    dx = sum(jnp.where(c % nx == p, d, 0) for p, d in enumerate(turn))
    mirror = jnp.where(2 * dx > nx, -1, 1)
    core = (mk + rk) % nk
    dz = (nz + mirror * i + core * half_z) % nz
    dy = (2 * ny + mirror * (u + i) + core * half_y) % ny
    source = (((mz + nz - dz) % nz * ny + (my + ny - dy) % ny) * nx + (mx + nx - dx) % nx) * nk + core
    before0 = jnp.sum(jnp.where(source < me, first, 0), axis=0, keepdims=True)
    before1 = jnp.sum(jnp.where(source < me, second, 0), axis=0, keepdims=True)
    total0 = jnp.sum(first, axis=0, keepdims=True)
    for j, offset in enumerate((before0, total0 + before1)):
        mine = jnp.sum(jnp.where(ids_col[:, j:j + 1] == lanes, offset, 0), axis=1, keepdims=True)
        wcol[:, j:j + 1] = jnp.where(mine + rcol[:, 2 + j:3 + j] < capacity, turned[:, 2 + j:3 + j], 0.0)

    acc0[...] = jnp.zeros_like(acc0)
    acc1[...] = jnp.zeros_like(acc1)
    xs[dense:wire, :] = jnp.zeros((wire - dense, model), BF16)

    def picks(g):
        cols = iota((tokens, wire), 1)
        wants = [rcol[:, j:j + 1] - g * dense for j in range(2)]
        return [ones((want == cols) & (cols < dense)) for want in wants]

    def combine(g, carry):
        wait_group(obuf, retbuf, r_send, r_recv, g, True)
        from_wire(retbuf, g, xs)
        for pick, acc in zip(picks(g), (acc0, acc1)):
            for b in range(4):
                part = slice(b * step, (b + 1) * step)
                acc[:, part] += jnp.dot(pick, xs[:, part], preferred_element_type=F32)
        return carry
    lax.fori_loop(0, ng - 1, combine, 0)

    last = ng - 1
    wait_group(obuf, retbuf, r_send, r_recv, last, True)
    from_wire(retbuf, last, xs)
    pick0, pick1 = picks(last)
    leaving = []
    for b in range(4):
        part = slice(b * step, (b + 1) * step)
        first = acc0[:, part] + jnp.dot(pick0, xs[:, part], preferred_element_type=F32)
        second = acc1[:, part] + jnp.dot(pick1, xs[:, part], preferred_element_type=F32)
        total[:, part] = wcol[:, 0:1] * first + wcol[:, 1:2] * second
        leave = pltpu.make_async_copy(total.at[:, part], out.at[:, part], o_sem.at[b])
        leave.start()
        leaving.append(leave)

    for leave in leaving:
        leave.wait()

    def drain(g, carry):
        wait_group(outbuf, inbuf, d_send, d_recv, g, False)
        wait_group(obuf, retbuf, r_send, r_recv, g, False)
        return carry
    lax.fori_loop(0, ng, drain, 0)


def torus(n):
    return (4, 4, 4, 2) if n == 128 else (2, 2, 2, 2)


def solution(mesh):
    n = mesh.shape["expert"]
    row_spec = P(("data", "expert"), None)
    weight_spec = P("expert", None, None)
    dims = torus(n)

    def device_step(token_rows, expert_ids, gate_weights, w_in, w_out):
        tokens, model = token_rows.shape
        hidden = w_in.shape[2]
        nc, ng = dims[0] * dims[1], dims[2] * dims[3]
        wire, dense = nc * WIRE_ROWS, nc * SLOTS
        width = SLOTS * model // WIRE_ROWS
        capacity = n * (tokens * 2 // n)
        hbm = pl.BlockSpec(memory_space=pltpu.HBM)
        dma = pltpu.SemaphoreType.DMA
        mixed = pl.pallas_call(
            functools.partial(moe_kernel, dims, capacity),
            out_shape=jax.ShapeDtypeStruct((tokens, model), F32),
            in_specs=[hbm] * 5,
            out_specs=hbm,
            scratch_shapes=[
                pltpu.VMEM((2, tokens), I32),
                pltpu.VMEM((2, tokens), F32),
                pltpu.VMEM((tokens, model), BF16),
                pltpu.VMEM((ng * wire, width), BF16),
                pltpu.VMEM((ng * wire, width), BF16),
                pltpu.VMEM((ng * wire, width), BF16),
                pltpu.VMEM((ng * wire, width), BF16),
                pltpu.VMEM((n, 1, n), I32),
                pltpu.VMEM((model, hidden), BF16),
                pltpu.VMEM((hidden, model), BF16),
                pltpu.VMEM((wire, width), BF16),
                pltpu.VMEM((wire, model), BF16),
                pltpu.VMEM((dense, hidden), BF16),
                pltpu.VMEM((tokens, model), F32),
                pltpu.VMEM((tokens, model), F32),
                pltpu.VMEM((tokens, model), F32),
                pltpu.VMEM((wire, wire), BF16),
                pltpu.VMEM((wire, wire), BF16),
                pltpu.VMEM((2, tokens), I32),
                pltpu.VMEM((tokens, 4), I32),
                pltpu.VMEM((tokens, 2), F32),
                pltpu.VMEM((8, tokens), F32),
                pltpu.VMEM((tokens, 8), F32),
                dma((5,)), dma((4,)), dma((1,)), dma((1,)), dma((ng,)), dma((ng,)), dma((ng,)), dma((ng,)),
            ],
            compiler_params=pltpu.CompilerParams(has_side_effects=True, collective_id=0, vmem_limit_bytes=VMEM_LIMIT),
        )(expert_ids.T, gate_weights.T, token_rows, w_in, w_out)
        return (token_rows.astype(F32) + mixed).astype(BF16)

    return jax.shard_map(device_step, mesh=mesh, in_specs=(row_spec, row_spec, row_spec, weight_spec, weight_spec), out_specs=row_spec, check_vma=False)
```

```python
import functools

import jax
import jax.numpy as jnp
from jax import lax
from jax.experimental import pallas as pl
from jax.experimental.pallas import tpu as pltpu
from jax.sharding import PartitionSpec as P

SLOTS = 14
WIRE_ROWS = 16
BF16 = jnp.bfloat16
F32 = jnp.float32
I32 = jnp.int32
VMEM_LIMIT = 60 * 1024 * 1024
XORDER = {4: (2, 1, 0, 3), 2: (1, 0)}


def moe_kernel(dims, capacity, ids_hbm, gates_hbm, x_hbm, win_hbm, wout_hbm, out,
               ids_row, gates_row, x, outbuf, inbuf, obuf, retbuf, cbuf, win, wout, st, xs, hs, acc0, acc1, tmat, tinv, rrow, rcol, wcol, flat, turned,
               w_sem, c_send, c_recv, f_send, f_recv, d_send, d_recv, r_send, r_recv):
    nz, ny, nx, nk = dims
    n = nz * ny * nx * nk
    nc, ng = nz * ny, nx * nk
    tokens, model = x_hbm.shape
    hidden = win.shape[1]
    dense = SLOTS * nc
    wire = WIRE_ROWS * nc
    half, quarter, eighth = model // 2, model // 4, model // 8
    width = SLOTS * model // WIRE_ROWS
    me = lax.axis_index("expert")
    mk = lax.rem(me, nk)
    mx = lax.rem(lax.div(me, nk), nx)
    my = lax.rem(lax.div(me, nk * nx), ny)
    mz = lax.div(me, nk * nx * ny)

    half_z, half_y = nz // 2, ny // 2
    turn = XORDER[nx]

    def each_peer(g, sign, act):
        u, rk = lax.div(g, nk), lax.rem(g, nk)
        core = mk if sign > 0 else lax.rem(mk + rk, nk)
        base = lax.rem(mk + rk, nk)
        parts = {}
        for c in range(nc):
            i, dx = c // nx, turn[c % nx]
            mirror = -1 if 2 * dx > nx else 1
            if (i, mirror) not in parts:
                dz = lax.rem(nz + mirror * i + core * half_z, nz)
                dy = lax.rem(2 * ny + mirror * (u + i) + core * half_y, ny)
                z = lax.rem(mz + nz + sign * dz, nz)
                y = lax.rem(my + ny + sign * dy, ny)
                parts[i, mirror] = (z * ny + y) * (nx * nk) + base
            device = parts[i, mirror] + lax.rem(mx + nx + sign * dx, nx) * nk
            if dx == 0:
                @pl.when(device != me)
                def _():
                    act(c, device)
            else:
                act(c, device)
    own = (mk * half_z) * nx + turn.index(0)
    own_rows = pl.ds(pl.multiple_of(own * WIRE_ROWS, WIRE_ROWS), WIRE_ROWS)

    def start_group(src, dst, ssem, rsem, g, sign):
        def act(c, device):
            rows = pl.ds(pl.multiple_of(g * wire + c * WIRE_ROWS, WIRE_ROWS), WIRE_ROWS)
            pltpu.make_async_remote_copy(src_ref=src.at[rows], dst_ref=dst.at[rows], send_sem=ssem.at[g], recv_sem=rsem.at[g],
                                         device_id={"expert": device}, device_id_type=pl.DeviceIdType.MESH).start()
        each_peer(g, sign, act)

    def wait_group(src, dst, ssem, rsem, g, recv):
        def wait(first, count):
            rows = pl.ds(pl.multiple_of(first, WIRE_ROWS), count)
            copy = pltpu.make_async_remote_copy(src_ref=src.at[rows], dst_ref=dst.at[rows], send_sem=ssem.at[g], recv_sem=rsem.at[g],
                                                device_id={"expert": me}, device_id_type=pl.DeviceIdType.MESH)
            copy.wait_recv() if recv else copy.wait_send()

        @pl.when(g == 0)
        def _():
            wait(WIRE_ROWS, wire - WIRE_ROWS)

        @pl.when(g > 0)
        def _():
            wait(g * wire, wire)

    def row_of(ids, slot):
        dz = (ids // (nk * nx * ny) + nz - mz + mk * half_z) % nz
        dy = ((ids // (nk * nx)) % ny + ny - my + mk * half_y) % ny
        dx = ((ids // nk) % nx + nx - mx) % nx
        dk = (ids % nk + nk - mk) % nk
        flip = 2 * dx > nx
        i = jnp.where(flip, (nz - dz) % nz, dz)
        u = (jnp.where(flip, (ny - dy) % ny, dy) + ny - i) % ny
        q = sum(jnp.where(dx == d, p, 0) for p, d in enumerate(turn))
        return (u * nk + dk) * dense + slot * nc + i * nx + q

    def iota(shape, dim):
        return lax.broadcasted_iota(I32, shape, dim)

    def ones(mask):
        return jnp.where(mask, jnp.float32(1.0), jnp.float32(0.0)).astype(BF16)

    fetch = [pltpu.make_async_copy(src, dst, w_sem.at[i]) for i, (src, dst) in enumerate((
        (ids_hbm, ids_row), (gates_hbm, gates_row), (x_hbm, x), (win_hbm.at[0], win), (wout_hbm.at[0], wout)))]
    for copy in fetch:
        copy.start()

    barrier = pltpu.get_barrier_semaphore()

    def hello(i, carry):
        pl.semaphore_signal(barrier, inc=1, device_id={"expert": lax.rem(me + i, n)}, device_id_type=pl.DeviceIdType.MESH)
        return carry
    lax.fori_loop(1, n, hello, 0, unroll=4)
    fetch[0].wait()
    fetch[1].wait()

    flat[0:2, :] = ids_row[...].astype(F32)
    flat[2:4, :] = gates_row[...]
    flat[4:8, :] = jnp.zeros((4, tokens), F32)
    turned[...] = flat[...].T
    ids_col = turned[:, 0:2].astype(I32)

    earlier = iota((tokens, tokens), 0) < iota((tokens, tokens), 1)
    row_ids = [ids_row[j:j + 1, :] for j in range(2)]

    def lane_rank(j, other, mask):
        same = ids_col[:, j:j + 1] == row_ids[other]
        if mask:
            same = same & earlier
        return jnp.sum(jnp.where(same, 1, 0).astype(I32), axis=0, keepdims=True)
    rrow[0:1, :] = row_of(row_ids[0], lane_rank(0, 0, True))
    rrow[1:2, :] = row_of(row_ids[1], lane_rank(1, 1, True) + lane_rank(0, 1, False))

    swap = (iota((wire, wire), 0) % WIRE_ROWS) * nc + iota((wire, wire), 0) // WIRE_ROWS
    tmat[...] = ones(swap == iota((wire, wire), 1))
    swap = (iota((wire, wire), 1) % WIRE_ROWS) * nc + iota((wire, wire), 1) // WIRE_ROWS
    tinv[...] = ones(swap == iota((wire, wire), 0))

    step = quarter

    def stack(b, block):
        h, r = (b * quarter) // half, (b * quarter) % half
        st[h * 8 * nc:(h + 1) * 8 * nc, r:r + quarter] = block[:8 * nc]
        st[b * 4 * nc:(b + 1) * 4 * nc, half:half + quarter] = block[8 * nc:12 * nc]
        for o in range(2):
            st[(2 * b + o) * 2 * nc:(2 * b + o + 1) * 2 * nc, half + quarter:width] = block[12 * nc:, o * eighth:(o + 1) * eighth]

    def to_wire(buf, g):
        rows = pl.ds(pl.multiple_of(g * wire, WIRE_ROWS), wire)
        for lo, hi in ((0, quarter), (quarter, half), (half, half + quarter), (half + quarter, width)):
            buf[rows, lo:hi] = jnp.dot(tmat[...], st[:, lo:hi], preferred_element_type=F32).astype(BF16)

    def from_wire(buf, g, dst):
        rows = pl.ds(pl.multiple_of(g * wire, WIRE_ROWS), wire)
        for r in (0, quarter):
            part = jnp.dot(tinv[...], buf[rows, r:r + quarter], preferred_element_type=F32).astype(BF16)
            dst[0:8 * nc, r:r + quarter] = part[:8 * nc]
            dst[0:8 * nc, half + r:half + r + quarter] = part[8 * nc:]
        part = jnp.dot(tinv[...], buf[rows, half:half + quarter], preferred_element_type=F32).astype(BF16)
        for q in range(4):
            dst[8 * nc:12 * nc, q * quarter:(q + 1) * quarter] = part[q * 4 * nc:(q + 1) * 4 * nc]
        part = jnp.dot(tinv[...], buf[rows, half + quarter:width], preferred_element_type=F32).astype(BF16)
        for o in range(8):
            dst[12 * nc:dense, o * eighth:(o + 1) * eighth] = part[o * 2 * nc:(o + 1) * 2 * nc]

    def build(g, carry):
        rows = iota((dense, tokens), 0) + g * dense
        pick = ones((rows == rrow[0:1, :]) | (rows == rrow[1:2, :]))
        for b in range(4):
            block = jnp.dot(pick, x[:, b * step:(b + 1) * step], preferred_element_type=F32).astype(BF16)
            stack(b, block)
        to_wire(outbuf, g)
        return carry
    fetch[2].wait()
    lax.fori_loop(0, ng // 2, build, 0)

    lanes = iota((tokens, n), 1)
    count = [jnp.sum(jnp.where(ids_col[:, j:j + 1] == lanes, 1, 0).astype(I32), axis=0, keepdims=True) for j in range(2)]
    cbuf[own] = count[0] + count[1] * 65536

    pl.semaphore_wait(barrier, n - 1)

    def dispatch(g, carry):
        start_group(outbuf, inbuf, d_send, d_recv, g, 1)
        return carry
    lax.fori_loop(0, ng // 2, dispatch, 0)

    def build_dispatch(g, carry):
        return dispatch(g, build(g, carry))
    lax.fori_loop(ng // 2, ng, build_dispatch, 0)

    def send_counts(u, carry):
        g = u * nk

        def act(c, device):
            pltpu.make_async_remote_copy(src_ref=cbuf.at[own], dst_ref=cbuf.at[g * nc + c], send_sem=c_send.at[0], recv_sem=c_recv.at[0],
                                         device_id={"expert": device}, device_id_type=pl.DeviceIdType.MESH).start()
        each_peer(g, 1, act)
        return carry
    lax.fori_loop(0, ng // nk, send_counts, 0)
    inbuf[own_rows, :] = outbuf[own_rows, :]

    later = iota((tokens, tokens), 1) < iota((tokens, tokens), 0)

    def sub_rank(j, other, mask):
        same = ids_col[:, other:other + 1] == row_ids[j]
        if mask:
            same = same & later
        return jnp.sum(jnp.where(same, 1, 0).astype(I32), axis=1, keepdims=True)
    rank0 = sub_rank(0, 0, True)
    rank1 = sub_rank(1, 1, True)
    rcol[:, 0:1] = row_of(ids_col[:, 0:1], rank0)
    rcol[:, 1:2] = row_of(ids_col[:, 1:2], rank1 + sub_rank(0, 1, False))
    rcol[:, 2:3] = rank0
    rcol[:, 3:4] = rank1

    fetch[3].wait()
    fetch[4].wait()

    def expert(g, carry):
        wait_group(outbuf, inbuf, d_send, d_recv, g, True)
        from_wire(inbuf, g, xs)
        for b in range(4):
            cols = slice(b * hidden // 4, (b + 1) * hidden // 4)
            pre = jnp.dot(xs[0:dense, :], win[:, cols], preferred_element_type=F32)
            hs[:, cols] = jax.nn.gelu(pre).astype(BF16)
        for b in range(4):
            block = jnp.dot(hs[...], wout[:, b * step:(b + 1) * step], preferred_element_type=F32).astype(BF16)
            stack(b, block)
        to_wire(obuf, g)
        start_group(obuf, retbuf, r_send, r_recv, g, -1)
        return carry
    lax.fori_loop(0, ng, expert, 0)
    retbuf[own_rows, :] = obuf[own_rows, :]

    near = pl.ds(0, n // nk - 1)
    pltpu.make_async_remote_copy(src_ref=cbuf.at[near], dst_ref=cbuf.at[near], send_sem=c_send.at[0], recv_sem=c_recv.at[0],
                                 device_id={"expert": me}, device_id_type=pl.DeviceIdType.MESH).wait()
    hand = [pltpu.make_async_remote_copy(src_ref=cbuf.at[pl.ds(u * nk * nc, nc)], dst_ref=cbuf.at[pl.ds((u * nk + 1) * nc, nc)],
                                         send_sem=f_send.at[u], recv_sem=f_recv.at[u],
                                         device_id={"expert": me - mk + lax.rem(mk + 1, nk)}, device_id_type=pl.DeviceIdType.MESH)
            for u in range(ng // nk)]
    for copy in hand:
        copy.start()

    acc0[...] = jnp.zeros_like(acc0)
    acc1[...] = jnp.zeros_like(acc1)
    xs[dense:wire, :] = jnp.zeros((wire - dense, model), BF16)

    def picks(g):
        cols = iota((tokens, wire), 1)
        wants = [rcol[:, j:j + 1] - g * dense for j in range(2)]
        return [ones((want == cols) & (cols < dense)) for want in wants]

    def combine(g, carry):
        wait_group(obuf, retbuf, r_send, r_recv, g, True)
        from_wire(retbuf, g, xs)
        for pick, acc in zip(picks(g), (acc0, acc1)):
            for b in range(4):
                part = slice(b * step, (b + 1) * step)
                acc[:, part] += jnp.dot(pick, xs[:, part], preferred_element_type=F32)
        return carry
    lax.fori_loop(0, ng // 2, combine, 0)

    for copy in hand:
        copy.wait()
    packed = cbuf[...].reshape(n, n)
    second = packed // 65536
    first = packed - second * 65536
    slot = iota((n, n), 0)
    g, c = slot // nc, slot % nc
    u, rk, i = g // nk, g % nk, c // nx
    dx = sum(jnp.where(c % nx == p, d, 0) for p, d in enumerate(turn))
    mirror = jnp.where(2 * dx > nx, -1, 1)
    core = (mk + rk) % nk
    dz = (nz + mirror * i + core * half_z) % nz
    dy = (2 * ny + mirror * (u + i) + core * half_y) % ny
    source = (((mz + nz - dz) % nz * ny + (my + ny - dy) % ny) * nx + (mx + nx - dx) % nx) * nk + core
    before0 = jnp.sum(jnp.where(source < me, first, 0), axis=0, keepdims=True)
    before1 = jnp.sum(jnp.where(source < me, second, 0), axis=0, keepdims=True)
    total0 = jnp.sum(first, axis=0, keepdims=True)
    for j, offset in enumerate((before0, total0 + before1)):
        mine = jnp.sum(jnp.where(ids_col[:, j:j + 1] == lanes, offset, 0), axis=1, keepdims=True)
        wcol[:, j:j + 1] = jnp.where(mine + rcol[:, 2 + j:3 + j] < capacity, turned[:, 2 + j:3 + j], 0.0)

    lax.fori_loop(ng // 2, ng - 1, combine, 0)

    last = ng - 1
    wait_group(obuf, retbuf, r_send, r_recv, last, True)
    from_wire(retbuf, last, xs)
    pick0, pick1 = picks(last)
    for b in range(4):
        part = slice(b * step, (b + 1) * step)
        first = acc0[:, part] + jnp.dot(pick0, xs[:, part], preferred_element_type=F32)
        second = acc1[:, part] + jnp.dot(pick1, xs[:, part], preferred_element_type=F32)
        out[:, part] = (x[:, part].astype(F32) + wcol[:, 0:1] * first + wcol[:, 1:2] * second).astype(BF16)

    def drain(g, carry):
        wait_group(outbuf, inbuf, d_send, d_recv, g, False)
        wait_group(obuf, retbuf, r_send, r_recv, g, False)
        return carry
    lax.fori_loop(0, ng, drain, 0)


def torus(n):
    return (4, 4, 4, 2) if n == 128 else (2, 2, 2, 2)


def solution(mesh):
    n = mesh.shape["expert"]
    row_spec = P(("data", "expert"), None)
    weight_spec = P("expert", None, None)
    dims = torus(n)

    def device_step(token_rows, expert_ids, gate_weights, w_in, w_out):
        tokens, model = token_rows.shape
        hidden = w_in.shape[2]
        nc, ng = dims[0] * dims[1], dims[2] * dims[3]
        wire, dense = nc * WIRE_ROWS, nc * SLOTS
        width = SLOTS * model // WIRE_ROWS
        capacity = n * (tokens * 2 // n)
        vmem = pl.BlockSpec(memory_space=pltpu.VMEM)
        hbm = pl.BlockSpec(memory_space=pltpu.HBM)
        dma = pltpu.SemaphoreType.DMA
        return pl.pallas_call(
            functools.partial(moe_kernel, dims, capacity),
            out_shape=pltpu.VMEM((tokens, model), BF16),
            in_specs=[hbm] * 5,
            out_specs=vmem,
            scratch_shapes=[
                pltpu.VMEM((2, tokens), I32),
                pltpu.VMEM((2, tokens), F32),
                pltpu.VMEM((tokens, model), BF16),
                pltpu.VMEM((ng * wire, width), BF16),
                pltpu.VMEM((ng * wire, width), BF16),
                pltpu.VMEM((ng * wire, width), BF16),
                pltpu.VMEM((ng * wire, width), BF16),
                pltpu.VMEM((n, 1, n), I32),
                pltpu.VMEM((model, hidden), BF16),
                pltpu.VMEM((hidden, model), BF16),
                pltpu.VMEM((wire, width), BF16),
                pltpu.VMEM((wire, model), BF16),
                pltpu.VMEM((dense, hidden), BF16),
                pltpu.VMEM((tokens, model), F32),
                pltpu.VMEM((tokens, model), F32),
                pltpu.VMEM((wire, wire), BF16),
                pltpu.VMEM((wire, wire), BF16),
                pltpu.VMEM((2, tokens), I32),
                pltpu.VMEM((tokens, 4), I32),
                pltpu.VMEM((tokens, 2), F32),
                pltpu.VMEM((8, tokens), F32),
                pltpu.VMEM((tokens, 8), F32),
                dma((5,)), dma((1,)), dma((1,)), dma((ng // dims[3],)), dma((ng // dims[3],)), dma((ng,)), dma((ng,)), dma((ng,)), dma((ng,)),
            ],
            compiler_params=pltpu.CompilerParams(has_side_effects=True, collective_id=0, vmem_limit_bytes=VMEM_LIMIT),
        )(expert_ids.T, gate_weights.T, token_rows, w_in, w_out)

    return jax.shard_map(device_step, mesh=mesh, in_specs=(row_spec, row_spec, row_spec, weight_spec, weight_spec), out_specs=row_spec, check_vma=False)
```

```python
import functools

import jax
import jax.numpy as jnp
from jax import lax
from jax.experimental import pallas as pl
from jax.experimental.pallas import tpu as pltpu
from jax.sharding import PartitionSpec as P

SLOTS = 14
WIRE_ROWS = 16
BF16 = jnp.bfloat16
F32 = jnp.float32
I32 = jnp.int32
VMEM_LIMIT = 60 * 1024 * 1024
XORDER = {4: (2, 1, 0, 3), 2: (1, 0)}


def moe_kernel(dims, capacity, ids_hbm, gates_hbm, x_hbm, win_hbm, wout_hbm, out,
               ids_row, gates_row, x, outbuf, inbuf, obuf, retbuf, cbuf, win, wout, st, xs, hs, acc0, acc1, tmat, tinv, rrow, rcol, wcol, flat, turned,
               w_sem, c_send, c_recv, f_send, f_recv, d_send, d_recv, r_send, r_recv):
    nz, ny, nx, nk = dims
    n = nz * ny * nx * nk
    nc, ng = nz * ny, nx * nk
    tokens, model = x_hbm.shape
    hidden = win.shape[1]
    dense = SLOTS * nc
    wire = WIRE_ROWS * nc
    half, quarter, eighth = model // 2, model // 4, model // 8
    width = SLOTS * model // WIRE_ROWS
    me = lax.axis_index("expert")
    mk = lax.rem(me, nk)
    mx = lax.rem(lax.div(me, nk), nx)
    my = lax.rem(lax.div(me, nk * nx), ny)
    mz = lax.div(me, nk * nx * ny)

    half_z, half_y = nz // 2, ny // 2
    turn = XORDER[nx]

    def each_peer(g, sign, act):
        u, rk = lax.div(g, nk), lax.rem(g, nk)
        core = mk if sign > 0 else lax.rem(mk + rk, nk)
        base = lax.rem(mk + rk, nk)
        parts = {}
        for c in range(nc):
            i, dx = c // nx, turn[c % nx]
            mirror = -1 if 2 * dx > nx else 1
            if (i, mirror) not in parts:
                dz = lax.rem(nz + mirror * i + core * half_z, nz)
                dy = lax.rem(2 * ny + mirror * (u + i) + core * half_y, ny)
                z = lax.rem(mz + nz + sign * dz, nz)
                y = lax.rem(my + ny + sign * dy, ny)
                parts[i, mirror] = (z * ny + y) * (nx * nk) + base
            device = parts[i, mirror] + lax.rem(mx + nx + sign * dx, nx) * nk
            if dx == 0:
                @pl.when(device != me)
                def _():
                    act(c, device)
            else:
                act(c, device)
    own = (mk * half_z) * nx + turn.index(0)
    own_rows = pl.ds(pl.multiple_of(own * WIRE_ROWS, WIRE_ROWS), WIRE_ROWS)

    def start_group(src, dst, ssem, rsem, g, sign):
        def act(c, device):
            rows = pl.ds(pl.multiple_of(g * wire + c * WIRE_ROWS, WIRE_ROWS), WIRE_ROWS)
            pltpu.make_async_remote_copy(src_ref=src.at[rows], dst_ref=dst.at[rows], send_sem=ssem.at[g], recv_sem=rsem.at[g],
                                         device_id={"expert": device}, device_id_type=pl.DeviceIdType.MESH).start()
        each_peer(g, sign, act)

    def wait_group(src, dst, ssem, rsem, g, recv):
        def wait(first, count):
            rows = pl.ds(pl.multiple_of(first, WIRE_ROWS), count)
            copy = pltpu.make_async_remote_copy(src_ref=src.at[rows], dst_ref=dst.at[rows], send_sem=ssem.at[g], recv_sem=rsem.at[g],
                                                device_id={"expert": me}, device_id_type=pl.DeviceIdType.MESH)
            copy.wait_recv() if recv else copy.wait_send()

        @pl.when(g == 0)
        def _():
            wait(WIRE_ROWS, wire - WIRE_ROWS)

        @pl.when(g > 0)
        def _():
            wait(g * wire, wire)

    def row_of(ids, slot):
        dz = (ids // (nk * nx * ny) + nz - mz + mk * half_z) % nz
        dy = ((ids // (nk * nx)) % ny + ny - my + mk * half_y) % ny
        dx = ((ids // nk) % nx + nx - mx) % nx
        dk = (ids % nk + nk - mk) % nk
        flip = 2 * dx > nx
        i = jnp.where(flip, (nz - dz) % nz, dz)
        u = (jnp.where(flip, (ny - dy) % ny, dy) + ny - i) % ny
        q = sum(jnp.where(dx == d, p, 0) for p, d in enumerate(turn))
        return (u * nk + dk) * dense + slot * nc + i * nx + q

    def iota(shape, dim):
        return lax.broadcasted_iota(I32, shape, dim)

    def ones(mask):
        return jnp.where(mask, jnp.float32(1.0), jnp.float32(0.0)).astype(BF16)

    fetch = [pltpu.make_async_copy(src, dst, w_sem.at[i]) for i, (src, dst) in enumerate((
        (ids_hbm, ids_row), (gates_hbm, gates_row), (x_hbm, x), (win_hbm.at[0], win), (wout_hbm.at[0], wout)))]
    for copy in fetch:
        copy.start()

    barrier = pltpu.get_barrier_semaphore()

    def hello(i, carry):
        pl.semaphore_signal(barrier, inc=1, device_id={"expert": lax.rem(me + i, n)}, device_id_type=pl.DeviceIdType.MESH)
        return carry
    far = n // 2 - n // 32
    lax.fori_loop(far, n, hello, 0, unroll=4)
    lax.fori_loop(1, far, hello, 0, unroll=4)
    fetch[0].wait()
    fetch[1].wait()

    flat[0:2, :] = ids_row[...].astype(F32)
    flat[2:4, :] = gates_row[...]
    flat[4:8, :] = jnp.zeros((4, tokens), F32)
    turned[...] = flat[...].T
    ids_col = turned[:, 0:2].astype(I32)

    earlier = iota((tokens, tokens), 0) < iota((tokens, tokens), 1)
    row_ids = [ids_row[j:j + 1, :] for j in range(2)]

    def lane_rank(j, other, mask):
        same = ids_col[:, j:j + 1] == row_ids[other]
        if mask:
            same = same & earlier
        return jnp.sum(jnp.where(same, 1, 0).astype(I32), axis=0, keepdims=True)
    rrow[0:1, :] = row_of(row_ids[0], lane_rank(0, 0, True))
    rrow[1:2, :] = row_of(row_ids[1], lane_rank(1, 1, True) + lane_rank(0, 1, False))

    swap = (iota((wire, wire), 0) % WIRE_ROWS) * nc + iota((wire, wire), 0) // WIRE_ROWS
    tmat[...] = ones(swap == iota((wire, wire), 1))
    swap = (iota((wire, wire), 1) % WIRE_ROWS) * nc + iota((wire, wire), 1) // WIRE_ROWS
    tinv[...] = ones(swap == iota((wire, wire), 0))

    step = quarter

    def stack(b, block):
        h, r = (b * quarter) // half, (b * quarter) % half
        st[h * 8 * nc:(h + 1) * 8 * nc, r:r + quarter] = block[:8 * nc]
        st[b * 4 * nc:(b + 1) * 4 * nc, half:half + quarter] = block[8 * nc:12 * nc]
        for o in range(2):
            st[(2 * b + o) * 2 * nc:(2 * b + o + 1) * 2 * nc, half + quarter:width] = block[12 * nc:, o * eighth:(o + 1) * eighth]

    def to_wire(buf, g):
        rows = pl.ds(pl.multiple_of(g * wire, WIRE_ROWS), wire)
        for lo, hi in ((0, quarter), (quarter, half), (half, half + quarter), (half + quarter, width)):
            buf[rows, lo:hi] = jnp.dot(tmat[...], st[:, lo:hi], preferred_element_type=F32).astype(BF16)

    def from_wire(buf, g, dst):
        rows = pl.ds(pl.multiple_of(g * wire, WIRE_ROWS), wire)
        for r in (0, quarter):
            part = jnp.dot(tinv[...], buf[rows, r:r + quarter], preferred_element_type=F32).astype(BF16)
            dst[0:8 * nc, r:r + quarter] = part[:8 * nc]
            dst[0:8 * nc, half + r:half + r + quarter] = part[8 * nc:]
        part = jnp.dot(tinv[...], buf[rows, half:half + quarter], preferred_element_type=F32).astype(BF16)
        for q in range(4):
            dst[8 * nc:12 * nc, q * quarter:(q + 1) * quarter] = part[q * 4 * nc:(q + 1) * 4 * nc]
        part = jnp.dot(tinv[...], buf[rows, half + quarter:width], preferred_element_type=F32).astype(BF16)
        for o in range(8):
            dst[12 * nc:dense, o * eighth:(o + 1) * eighth] = part[o * 2 * nc:(o + 1) * 2 * nc]

    def build(g, carry):
        rows = iota((dense, tokens), 0) + g * dense
        pick = ones((rows == rrow[0:1, :]) | (rows == rrow[1:2, :]))
        for b in range(4):
            block = jnp.dot(pick, x[:, b * step:(b + 1) * step], preferred_element_type=F32).astype(BF16)
            stack(b, block)
        to_wire(outbuf, g)
        return carry
    fetch[2].wait()
    lax.fori_loop(0, ng // 2, build, 0)

    lanes = iota((tokens, n), 1)
    count = [jnp.sum(jnp.where(ids_col[:, j:j + 1] == lanes, 1, 0).astype(I32), axis=0, keepdims=True) for j in range(2)]
    cbuf[own] = count[0] + count[1] * 65536

    pl.semaphore_wait(barrier, n - 1)

    def dispatch(g, carry):
        start_group(outbuf, inbuf, d_send, d_recv, g, 1)
        return carry
    lax.fori_loop(0, ng // 2, dispatch, 0)

    def build_dispatch(g, carry):
        return dispatch(g, build(g, carry))
    lax.fori_loop(ng // 2, ng, build_dispatch, 0)

    def send_counts(u, carry):
        g = u * nk

        def act(c, device):
            pltpu.make_async_remote_copy(src_ref=cbuf.at[own], dst_ref=cbuf.at[g * nc + c], send_sem=c_send.at[0], recv_sem=c_recv.at[0],
                                         device_id={"expert": device}, device_id_type=pl.DeviceIdType.MESH).start()
        each_peer(g, 1, act)
        return carry
    lax.fori_loop(0, ng // nk, send_counts, 0)
    inbuf[own_rows, :] = outbuf[own_rows, :]

    later = iota((tokens, tokens), 1) < iota((tokens, tokens), 0)

    def sub_rank(j, other, mask):
        same = ids_col[:, other:other + 1] == row_ids[j]
        if mask:
            same = same & later
        return jnp.sum(jnp.where(same, 1, 0).astype(I32), axis=1, keepdims=True)
    rank0 = sub_rank(0, 0, True)
    rank1 = sub_rank(1, 1, True)
    rcol[:, 0:1] = row_of(ids_col[:, 0:1], rank0)
    rcol[:, 1:2] = row_of(ids_col[:, 1:2], rank1 + sub_rank(0, 1, False))
    rcol[:, 2:3] = rank0
    rcol[:, 3:4] = rank1

    acc0[...] = jnp.zeros_like(acc0)
    acc1[...] = jnp.zeros_like(acc1)
    xs[dense:wire, :] = jnp.zeros((wire - dense, model), BF16)
    fetch[3].wait()
    fetch[4].wait()

    def expert(g, carry):
        wait_group(outbuf, inbuf, d_send, d_recv, g, True)
        from_wire(inbuf, g, xs)
        for b in range(4):
            cols = slice(b * hidden // 4, (b + 1) * hidden // 4)
            pre = jnp.dot(xs[0:dense, :], win[:, cols], preferred_element_type=F32)
            hs[:, cols] = jax.nn.gelu(pre).astype(BF16)
        for b in range(4):
            block = jnp.dot(hs[...], wout[:, b * step:(b + 1) * step], preferred_element_type=F32).astype(BF16)
            stack(b, block)
        to_wire(obuf, g)
        start_group(obuf, retbuf, r_send, r_recv, g, -1)
        return carry
    lax.fori_loop(0, ng, expert, 0)
    retbuf[own_rows, :] = obuf[own_rows, :]

    near = pl.ds(0, n // nk - 1)
    pltpu.make_async_remote_copy(src_ref=cbuf.at[near], dst_ref=cbuf.at[near], send_sem=c_send.at[0], recv_sem=c_recv.at[0],
                                 device_id={"expert": me}, device_id_type=pl.DeviceIdType.MESH).wait()
    hand = [pltpu.make_async_remote_copy(src_ref=cbuf.at[pl.ds(u * nk * nc, nc)], dst_ref=cbuf.at[pl.ds((u * nk + 1) * nc, nc)],
                                         send_sem=f_send.at[u], recv_sem=f_recv.at[u],
                                         device_id={"expert": me - mk + lax.rem(mk + 1, nk)}, device_id_type=pl.DeviceIdType.MESH)
            for u in range(ng // nk)]
    for copy in hand:
        copy.start()


    def picks(g):
        cols = iota((tokens, wire), 1)
        wants = [rcol[:, j:j + 1] - g * dense for j in range(2)]
        return [ones((want == cols) & (cols < dense)) for want in wants]

    def combine(g, carry):
        wait_group(obuf, retbuf, r_send, r_recv, g, True)
        from_wire(retbuf, g, xs)
        for pick, acc in zip(picks(g), (acc0, acc1)):
            for b in range(4):
                part = slice(b * step, (b + 1) * step)
                acc[:, part] += jnp.dot(pick, xs[:, part], preferred_element_type=F32)
        return carry
    lax.fori_loop(0, ng // 2, combine, 0)

    for copy in hand:
        copy.wait()
    packed = cbuf[...].reshape(n, n)
    second = packed // 65536
    first = packed - second * 65536
    slot = iota((n, n), 0)
    g, c = slot // nc, slot % nc
    u, rk, i = g // nk, g % nk, c // nx
    dx = sum(jnp.where(c % nx == p, d, 0) for p, d in enumerate(turn))
    mirror = jnp.where(2 * dx > nx, -1, 1)
    core = (mk + rk) % nk
    dz = (nz + mirror * i + core * half_z) % nz
    dy = (2 * ny + mirror * (u + i) + core * half_y) % ny
    source = (((mz + nz - dz) % nz * ny + (my + ny - dy) % ny) * nx + (mx + nx - dx) % nx) * nk + core
    before0 = jnp.sum(jnp.where(source < me, first, 0), axis=0, keepdims=True)
    before1 = jnp.sum(jnp.where(source < me, second, 0), axis=0, keepdims=True)
    total0 = jnp.sum(first, axis=0, keepdims=True)
    for j, offset in enumerate((before0, total0 + before1)):
        mine = jnp.sum(jnp.where(ids_col[:, j:j + 1] == lanes, offset, 0), axis=1, keepdims=True)
        wcol[:, j:j + 1] = jnp.where(mine + rcol[:, 2 + j:3 + j] < capacity, turned[:, 2 + j:3 + j], 0.0)

    lax.fori_loop(ng // 2, ng - 1, combine, 0)

    last = ng - 1
    wait_group(obuf, retbuf, r_send, r_recv, last, True)
    from_wire(retbuf, last, xs)
    pick0, pick1 = picks(last)
    for b in range(4):
        part = slice(b * step, (b + 1) * step)
        first = acc0[:, part] + jnp.dot(pick0, xs[:, part], preferred_element_type=F32)
        second = acc1[:, part] + jnp.dot(pick1, xs[:, part], preferred_element_type=F32)
        out[:, part] = (x[:, part].astype(F32) + wcol[:, 0:1] * first + wcol[:, 1:2] * second).astype(BF16)

    def drain(g, carry):
        wait_group(outbuf, inbuf, d_send, d_recv, g, False)
        wait_group(obuf, retbuf, r_send, r_recv, g, False)
        return carry
    lax.fori_loop(0, ng, drain, 0)


def torus(n):
    return (4, 4, 4, 2) if n == 128 else (2, 2, 2, 2)


def solution(mesh):
    n = mesh.shape["expert"]
    row_spec = P(("data", "expert"), None)
    weight_spec = P("expert", None, None)
    dims = torus(n)

    def device_step(token_rows, expert_ids, gate_weights, w_in, w_out):
        tokens, model = token_rows.shape
        hidden = w_in.shape[2]
        nc, ng = dims[0] * dims[1], dims[2] * dims[3]
        wire, dense = nc * WIRE_ROWS, nc * SLOTS
        width = SLOTS * model // WIRE_ROWS
        capacity = n * (tokens * 2 // n)
        vmem = pl.BlockSpec(memory_space=pltpu.VMEM)
        hbm = pl.BlockSpec(memory_space=pltpu.HBM)
        dma = pltpu.SemaphoreType.DMA
        return pl.pallas_call(
            functools.partial(moe_kernel, dims, capacity),
            out_shape=pltpu.VMEM((tokens, model), BF16),
            in_specs=[hbm] * 5,
            out_specs=vmem,
            scratch_shapes=[
                pltpu.VMEM((2, tokens), I32),
                pltpu.VMEM((2, tokens), F32),
                pltpu.VMEM((tokens, model), BF16),
                pltpu.VMEM((ng * wire, width), BF16),
                pltpu.VMEM((ng * wire, width), BF16),
                pltpu.VMEM((ng * wire, width), BF16),
                pltpu.VMEM((ng * wire, width), BF16),
                pltpu.VMEM((n, 1, n), I32),
                pltpu.VMEM((model, hidden), BF16),
                pltpu.VMEM((hidden, model), BF16),
                pltpu.VMEM((wire, width), BF16),
                pltpu.VMEM((wire, model), BF16),
                pltpu.VMEM((dense, hidden), BF16),
                pltpu.VMEM((tokens, model), F32),
                pltpu.VMEM((tokens, model), F32),
                pltpu.VMEM((wire, wire), BF16),
                pltpu.VMEM((wire, wire), BF16),
                pltpu.VMEM((2, tokens), I32),
                pltpu.VMEM((tokens, 4), I32),
                pltpu.VMEM((tokens, 2), F32),
                pltpu.VMEM((8, tokens), F32),
                pltpu.VMEM((tokens, 8), F32),
                dma((5,)), dma((1,)), dma((1,)), dma((ng // dims[3],)), dma((ng // dims[3],)), dma((ng,)), dma((ng,)), dma((ng,)), dma((ng,)),
            ],
            compiler_params=pltpu.CompilerParams(has_side_effects=True, collective_id=0, vmem_limit_bytes=VMEM_LIMIT),
        )(expert_ids.T, gate_weights.T, token_rows, w_in, w_out)

    return jax.shard_map(device_step, mesh=mesh, in_specs=(row_spec, row_spec, row_spec, weight_spec, weight_spec), out_specs=row_spec, check_vma=False)
```
